8 devices in a mesh: data: 2 (over z, y), tp: 4 (over x, core).
Axes of the slice: x: 2, y: 2, z: 1, core: 2. Of those that a mesh axis runs over, the one named last changes fastest.
Arguments:
- x_tokens: bfloat16 [512, 5120], P(('data', 'tp')), parts along dimension 0
- ln_gamma: float32 [5120], replicated
- w_qkv: bfloat16 [5120, 40, 384], P(None, 'tp')
- w_out: bfloat16 [40, 128, 5120], P('tp')
- w_up: bfloat16 [5120, 13824], P(None, 'tp')
- w_down: bfloat16 [13824, 5120], P('tp')
Outputs:
- output: bfloat16 [512, 5120], P(('data', 'tp')), parts along dimension 0
There are 2 independent parts. The reference program is written for one: setup_inputs(seed, part) draws one part's arguments, and reference() takes and returns one part's arrays. A program takes and returns all parts, laid end to end along the dimension named above; an argument that names none is the same for every part.
All inputs are finite; a program needn't handle non-finite values.
Results may differ from the reference program's by a relative error of at most 0.0027405.
Values are sent between devices in bfloat16 or wider.
A program may use at most 1 GiB of HBM per device.

```python
import math
import jax
import jax.numpy as jnp
from jax import lax

SEQ_LEN = 256
MODEL_DIM = 5120
FF_DIM = 13824
NUM_HEADS = 40
HEAD_DIM = MODEL_DIM // NUM_HEADS
BLOCK_ROWS = min(SEQ_LEN, 256)
N_BLOCKS = SEQ_LEN // BLOCK_ROWS
ATTN_SCALE = HEAD_DIM ** -0.5
LN_EPS = 1e-6
QK_GAIN = max(math.log(SEQ_LEN) - 2.0, 1.0) ** 0.25


def setup_inputs(seed: int = 0, part: int = 0) -> dict:
    rand_keys = jax.random.split(jax.random.key(seed), 6)
    tokens = jax.random.normal(jax.random.fold_in(rand_keys[0], part), (SEQ_LEN, MODEL_DIM), jnp.float32)
    ln_gain = 1.0 + 0.5 * jax.random.normal(rand_keys[1], (MODEL_DIM,), jnp.float32)
    qkv_gain = jnp.array([QK_GAIN, QK_GAIN, 1.0], jnp.float32).reshape(1, 1, 3, 1)
    w_qkv = jax.random.normal(rand_keys[2], (MODEL_DIM, NUM_HEADS, 3, HEAD_DIM), jnp.float32) * qkv_gain * MODEL_DIM ** -0.5
    w_out = jax.random.normal(rand_keys[3], (NUM_HEADS, HEAD_DIM, MODEL_DIM), jnp.float32) * (2.0 * MODEL_DIM ** -0.5)
    w_up = jax.random.normal(rand_keys[4], (MODEL_DIM, FF_DIM), jnp.float32) * MODEL_DIM ** -0.5
    w_down = jax.random.normal(rand_keys[5], (FF_DIM, MODEL_DIM), jnp.float32) * (1.5 * FF_DIM ** -0.5)
    return {
        "x_tokens": tokens.astype(jnp.bfloat16),
        "ln_gamma": ln_gain,
        "w_qkv": w_qkv.reshape(MODEL_DIM, NUM_HEADS, 3 * HEAD_DIM).astype(jnp.bfloat16),
        "w_out": w_out.astype(jnp.bfloat16),
        "w_up": w_up.astype(jnp.bfloat16),
        "w_down": w_down.astype(jnp.bfloat16),
    }


def layer_norm(row_vals, ln_gain):
    row_mean = jnp.mean(row_vals, axis=-1, keepdims=True)
    centered = row_vals - row_mean
    row_var = jnp.mean(centered * centered, axis=-1, keepdims=True)
    return centered * lax.rsqrt(row_var + LN_EPS) * ln_gain


def reference(x_tokens, ln_gamma, w_qkv, w_out, w_up, w_down):
    residual = x_tokens.astype(jnp.float32)
    normed = layer_norm(residual, ln_gamma).astype(jnp.bfloat16)

    def head_step(attn_acc, head_weights):
        wqkv_head, wout_head = head_weights
        qkv_rows = jnp.dot(normed, wqkv_head, preferred_element_type=jnp.float32).astype(jnp.bfloat16)
        query_rows = qkv_rows[:, :HEAD_DIM]
        key_trans = qkv_rows[:, HEAD_DIM:2 * HEAD_DIM].T
        value_rows = qkv_rows[:, 2 * HEAD_DIM:]

        def query_block(query_blk):
            scores = jnp.dot(query_blk, key_trans, preferred_element_type=jnp.float32) * ATTN_SCALE
            row_max = jnp.max(scores, axis=-1, keepdims=True)
            exp_scores = jnp.exp(scores - row_max)
            exp_sum = jnp.sum(exp_scores, axis=-1, keepdims=True)
            block_out = jnp.dot(exp_scores.astype(jnp.bfloat16), value_rows, preferred_element_type=jnp.float32)
            return (block_out / exp_sum).astype(jnp.bfloat16)

        head_out = lax.map(query_block, query_rows.reshape(N_BLOCKS, BLOCK_ROWS, HEAD_DIM)).reshape(SEQ_LEN, HEAD_DIM)
        return attn_acc + jnp.dot(head_out, wout_head, preferred_element_type=jnp.float32), None

    attn_init = jnp.zeros((SEQ_LEN, MODEL_DIM), jnp.float32)
    attn_sum = lax.scan(head_step, attn_init, (jnp.moveaxis(w_qkv, 1, 0), w_out))[0]

    def mlp_block(row_blk):
        pre_act = jnp.dot(row_blk, w_up, preferred_element_type=jnp.float32)
        hidden = jax.nn.gelu(pre_act, approximate=True).astype(jnp.bfloat16)
        return jnp.dot(hidden, w_down, preferred_element_type=jnp.float32)

    mlp_sum = lax.map(mlp_block, normed.reshape(N_BLOCKS, BLOCK_ROWS, MODEL_DIM)).reshape(SEQ_LEN, MODEL_DIM)
    return (residual + attn_sum + mlp_sum).astype(jnp.bfloat16)
```

```python
import jax
import jax.numpy as jnp
from jax import lax
from jax.experimental import pallas as pl
from jax.experimental.pallas import tpu as pltpu
from jax.sharding import PartitionSpec as P

LN_EPS = 1e-6
MESH = pl.DeviceIdType.MESH
F32 = jnp.float32
BF16 = jnp.bfloat16

KC = 512
NC = 512
U_SLOTS = 3
D_SLOTS = 3


def kernel(x_ref, g_ref, wqkv_ref, wup_ref, wout_ref, wdown_ref, y_ref,
           xn, acc_qkv, acc_up, wq_buf, wu_buf, wd_buf, act,
           snd_sib, rcv_sib, snd_x, rcv_x, mine,
           sem_wq, sem_wu, sem_wo, sem_wd,
           s_sib, r_sib, s_par, r_par, s_fwd, r_fwd,
           s_rs, r_rs, s_rx, r_rx):
    rows, dim = x_ref.shape
    heads, head_dim = wqkv_ref.shape[0], wqkv_ref.shape[2] // 3
    ff = wup_ref.shape[1]
    att = heads * head_dim
    nk, nj = dim // KC, dim // NC
    d = lax.axis_index("data")
    t = lax.axis_index("tp")
    sib = (d, t + 1 - 2 * (t % 2))
    par = (d, (t + 2) % 4)
    scale = head_dim ** -0.5

    bar = pltpu.get_barrier_semaphore()
    for peer in (sib, par):
        pl.semaphore_signal(bar, inc=1, device_id=peer, device_id_type=MESH)

    def up_copies(k, slot):
        rows_k = pl.ds(k * KC, KC)
        return (
            pltpu.make_async_copy(wqkv_ref.at[:, rows_k, :], wq_buf.at[slot], sem_wq.at[slot]),
            pltpu.make_async_copy(wup_ref.at[rows_k, :], wu_buf.at[slot], sem_wu.at[slot]),
        )

    def down_copies(j, slot):
        cols = pl.ds(j * NC, NC)
        return (
            pltpu.make_async_copy(wout_ref.at[:, cols], wd_buf.at[slot, pl.ds(0, att), :], sem_wo.at[slot]),
            pltpu.make_async_copy(wdown_ref.at[:, cols], wd_buf.at[slot, pl.ds(att, ff), :], sem_wd.at[slot]),
        )

    def remote(src, dst, ssem, rsem, peer):
        return pltpu.make_async_remote_copy(
            src_ref=src, dst_ref=dst, send_sem=ssem, recv_sem=rsem,
            device_id=peer, device_id_type=MESH)

    def blk(r):
        return pl.ds(r * rows, rows)

    def to_sib(k):
        return remote(xn.at[k, blk(0), :], xn.at[k, blk(1), :], s_sib.at[k], r_sib.at[k], sib)

    def to_par(k):
        return remote(xn.at[k, blk(0), :], xn.at[k, blk(2), :], s_par.at[k], r_par.at[k], par)

    def fwd(k):
        return remote(xn.at[k, blk(2), :], xn.at[k, blk(3), :], s_fwd.at[k], r_fwd.at[k], sib)

    def rs_sib(j):
        return remote(snd_sib.at[j], rcv_sib.at[j], s_rs.at[j], r_rs.at[j], sib)

    def rs_x(j):
        return remote(snd_x.at[j], rcv_x.at[j], s_rx.at[j], r_rx.at[j], par)

    for k in range(U_SLOTS):
        for c in up_copies(k, k):
            c.start()

    @pl.loop(0, rows // 16)
    def _(i):
        r = pl.ds(pl.multiple_of(i * 16, 16), 16)
        v = x_ref[r, :].astype(F32)
        cen = v - jnp.mean(v, axis=-1, keepdims=True)
        var = jnp.mean(cen * cen, axis=-1, keepdims=True)
        n = (cen * lax.rsqrt(var + LN_EPS) * g_ref[...]).astype(BF16)
        for k in range(nk):
            xn[k, r, :] = n[:, k * KC:(k + 1) * KC]

    pl.semaphore_wait(bar, 2)

    @pl.loop(0, nk)
    def _(k):
        to_par(k).start()
        to_sib(k).start()

    acc_qkv[...] = jnp.zeros_like(acc_qkv)
    acc_up[...] = jnp.zeros_like(acc_up)

    to_par(0).wait_recv()
    fwd(0).start()

    @pl.loop(0, nk)
    def _(k):
        slot = k % U_SLOTS

        @pl.when(k + 1 < nk)
        def _():
            to_par(k + 1).wait_recv()
            fwd(k + 1).start()

        to_sib(k).wait_recv()
        fwd(k).wait_recv()
        cq, cu = up_copies(k, slot)
        cq.wait()
        xk = xn[k]
        pair = 2 * 3 * head_dim
        for h in range(0, heads, 2):
            w = jnp.concatenate([wq_buf[slot, h], wq_buf[slot, h + 1]], axis=1)
            sl = slice(h // 2 * pair, (h // 2 + 1) * pair)
            acc_qkv[:, sl] += jnp.dot(xk, w, preferred_element_type=F32)
        cu.wait()
        for n in range(0, ff, pair):
            sl = slice(n, min(n + pair, ff))
            acc_up[:, sl] += jnp.dot(xk, wu_buf[slot, :, sl], preferred_element_type=F32)

        @pl.when(k + U_SLOTS < nk)
        def _():
            for c in up_copies(k + U_SLOTS, slot):
                c.start()

        @pl.when(k + U_SLOTS >= nk)
        def _():
            j = k + U_SLOTS - nk
            for c in down_copies(j, j):
                c.start()

    for h in range(heads):
        o = h * 3 * head_dim
        q = acc_qkv[:, o:o + head_dim].astype(BF16)
        kk = acc_qkv[:, o + head_dim:o + 2 * head_dim].astype(BF16)
        vv = acc_qkv[:, o + 2 * head_dim:o + 3 * head_dim].astype(BF16)
        s = lax.dot_general(q, kk, (((1,), (1,)), ((), ())), preferred_element_type=F32) * scale
        e = jnp.exp(s - jnp.max(s, axis=-1, keepdims=True))
        l = jnp.sum(e, axis=-1, keepdims=True)
        ov = jnp.dot(e.astype(BF16), vv, preferred_element_type=F32)
        act[:, h * head_dim:(h + 1) * head_dim] = (ov / l).astype(BF16)

    n_rows = act.shape[0]

    @pl.loop(0, n_rows // 16)
    def _(i):
        r = pl.ds(pl.multiple_of(i * 16, 16), 16)
        act[r, att:] = jax.nn.gelu(acc_up[r, :], approximate=True).astype(BF16)

    def combine(j):
        rs_sib(j).wait_recv()
        snd_x[j] = snd_x[j] + rcv_sib[j, 0]
        mine[j] = mine[j] + rcv_sib[j, 1]

    @pl.loop(0, nj)
    def _(j):
        slot = j % D_SLOTS
        co, cd = down_copies(j, slot)
        co.wait()
        cd.wait()
        p = jnp.dot(act[...], wd_buf[slot], preferred_element_type=F32)
        mine[j] = p[0:rows]
        snd_sib[j, 1] = p[rows:2 * rows]
        snd_x[j] = p[2 * rows:3 * rows]
        snd_sib[j, 0] = p[3 * rows:4 * rows]

        @pl.when(j > 0)
        def _():
            combine(j - 1)

        rs_sib(j).start()

        @pl.when(j > 0)
        def _():
            rs_x(j - 1).start()

        @pl.when(j + D_SLOTS < nj)
        def _():
            for c in down_copies(j + D_SLOTS, slot):
                c.start()

    combine(nj - 1)
    rs_x(nj - 1).start()

    for j in range(nj):
        rs_x(j).wait_recv()
        cols = slice(j * NC, (j + 1) * NC)
        y_ref[:, cols] = (x_ref[:, cols].astype(F32) + (mine[j] + rcv_x[j])).astype(BF16)

    @pl.loop(0, nk)
    def _(k):
        to_sib(k).wait_send()
        to_par(k).wait_send()
        fwd(k).wait_send()

    @pl.loop(0, nj)
    def _(j):
        rs_sib(j).wait_send()
        rs_x(j).wait_send()


def solution(mesh):
    def local_block(x_loc, ln_gamma, w_qkv, w_out, w_up, w_down):
        rows, dim = x_loc.shape
        heads, hd3 = w_qkv.shape[1:]
        att = heads * hd3 // 3
        ff = w_up.shape[1]
        seq = 4 * rows
        nk, nj = dim // KC, dim // NC
        vm = pl.BlockSpec(memory_space=pltpu.VMEM)
        hbm = pl.BlockSpec(memory_space=pl.ANY)
        dma = pltpu.SemaphoreType.DMA
        return pl.pallas_call(
            kernel,
            out_shape=jax.ShapeDtypeStruct((rows, dim), BF16),
            in_specs=[vm, vm, hbm, hbm, hbm, hbm],
            out_specs=vm,
            scratch_shapes=[
                pltpu.VMEM((nk, seq, KC), BF16),
                pltpu.VMEM((seq, heads * hd3), F32),
                pltpu.VMEM((seq, ff), F32),
                pltpu.VMEM((U_SLOTS, heads, KC, hd3), BF16),
                pltpu.VMEM((U_SLOTS, KC, ff), BF16),
                pltpu.VMEM((D_SLOTS, att + ff, NC), BF16),
                pltpu.VMEM((seq, att + ff), BF16),
                pltpu.VMEM((nj, 2, rows, NC), F32),
                pltpu.VMEM((nj, 2, rows, NC), F32),
                pltpu.VMEM((nj, rows, NC), F32),
                pltpu.VMEM((nj, rows, NC), F32),
                pltpu.VMEM((nj, rows, NC), F32),
                dma((U_SLOTS,)), dma((U_SLOTS,)), dma((D_SLOTS,)), dma((D_SLOTS,)),
                dma((nk,)), dma((nk,)), dma((nk,)), dma((nk,)), dma((nk,)), dma((nk,)),
                dma((nj,)), dma((nj,)), dma((nj,)), dma((nj,)),
            ],
            compiler_params=pltpu.CompilerParams(
                collective_id=0, has_side_effects=True, vmem_limit_bytes=66_900_000),
            cost_estimate=pl.CostEstimate(flops=32 * 10**9, bytes_accessed=125 * 10**6, transcendentals=10**6),
            name="block",
        )(x_loc, ln_gamma.reshape(1, dim), jnp.transpose(w_qkv, (1, 0, 2)), w_up,
          w_out.reshape(att, dim), w_down)

    row_spec = P(("data", "tp"), None)
    return jax.shard_map(
        local_block, mesh=mesh,
        in_specs=(row_spec, P(None), P(None, "tp", None), P("tp", None, None), P(None, "tp"), P("tp", None)),
        out_specs=row_spec, check_vma=False)
```

```python
import jax
import jax.numpy as jnp
from jax import lax
from jax.experimental import pallas as pl
from jax.experimental.pallas import tpu as pltpu
from jax.sharding import PartitionSpec as P

LN_EPS = 1e-6
MESH = pl.DeviceIdType.MESH
F32 = jnp.float32
BF16 = jnp.bfloat16

KC = 512
NC = 512
U_SLOTS = 4
LOCAL_FIRST = 3
D_SLOTS = 2


def kernel(x_hbm, g_ref, wqkv_ref, wup_ref, wout_ref, wdown_ref, y_ref,
           x_ref, stat, xn, acc_qkv, acc_up, wq_buf, wu_buf, wd_buf, act,
           snd_sc, rcv_sc, snd_so, rcv_so, snd_x, rcv_x, mine,
           sem_in, sem_wq, sem_wu, sem_wo, sem_wd,
           s_sib, r_sib, s_par, r_par, s_fwd, r_fwd,
           s_rc, r_rc, s_ro, r_ro, s_rx, r_rx):
    rows, dim = x_ref.shape
    heads, head_dim = wqkv_ref.shape[0], wqkv_ref.shape[2] // 3
    ff = wup_ref.shape[1]
    att = heads * head_dim
    nk, nj = dim // KC, dim // NC
    d = lax.axis_index("data")
    t = lax.axis_index("tp")
    sib = (d, t + 1 - 2 * (t % 2))
    par = (d, (t + 2) % 4)
    scale = head_dim ** -0.5
    near, far = slice(0, 2 * rows), slice(2 * rows, 4 * rows)

    x_in = pltpu.make_async_copy(x_hbm, x_ref, sem_in)
    x_in.start()

    bar = pltpu.get_barrier_semaphore()
    for peer in (sib, par):
        pl.semaphore_signal(bar, inc=1, device_id=peer, device_id_type=MESH)

    def q_copy(k, slot):
        return pltpu.make_async_copy(wqkv_ref.at[:, pl.ds(k * KC, KC), :], wq_buf.at[slot], sem_wq.at[slot])

    def u_copy(k, slot):
        return pltpu.make_async_copy(wup_ref.at[pl.ds(k * KC, KC), :], wu_buf.at[slot], sem_wu.at[slot])

    def down_copies(j, slot):
        cols = pl.ds(j * NC, NC)
        return (
            pltpu.make_async_copy(wout_ref.at[:, cols], wd_buf.at[slot, pl.ds(0, att), :], sem_wo.at[slot]),
            pltpu.make_async_copy(wdown_ref.at[:, cols], wd_buf.at[slot, pl.ds(att, ff), :], sem_wd.at[slot]),
        )

    def remote(src, dst, ssem, rsem, peer):
        return pltpu.make_async_remote_copy(
            src_ref=src, dst_ref=dst, send_sem=ssem, recv_sem=rsem,
            device_id=peer, device_id_type=MESH)

    def blk(r):
        return pl.ds(r * rows, rows)

    def to_sib(k):
        return remote(xn.at[k, blk(0), :], xn.at[k, blk(1), :], s_sib.at[k], r_sib.at[k], sib)

    def to_par(k):
        return remote(xn.at[k, blk(0), :], xn.at[k, blk(2), :], s_par.at[k], r_par.at[k], par)

    def fwd(k):
        return remote(xn.at[k, blk(2), :], xn.at[k, blk(3), :], s_fwd.at[k], r_fwd.at[k], sib)

    def rs_cross(j):
        return remote(snd_sc.at[j], rcv_sc.at[j], s_rc.at[j], r_rc.at[j], sib)

    def rs_own(j):
        return remote(snd_so.at[j], rcv_so.at[j], s_ro.at[j], r_ro.at[j], sib)

    def rs_x(j):
        return remote(snd_x.at[j], rcv_x.at[j], s_rx.at[j], r_rx.at[j], par)

    for k in range(U_SLOTS):
        q_copy(k, k).start()
        u_copy(k, k).start()

    x_in.wait()
    for i in range(rows // 16):
        r = slice(i * 16, (i + 1) * 16)
        v = x_ref[r, :].astype(F32)
        mean = jnp.mean(v, axis=-1, keepdims=True)
        cen = v - mean
        var = jnp.mean(cen * cen, axis=-1, keepdims=True)
        stat[0, r, :] = mean
        stat[1, r, :] = lax.rsqrt(var + LN_EPS)

    def normalize(k):
        c = slice(k * KC, (k + 1) * KC)
        cen = x_ref[:, c].astype(F32) - stat[0]
        xn[k, 0:rows, :] = (cen * stat[1] * g_ref[:, c]).astype(BF16)

    def send(k):
        to_par(k).start()
        to_sib(k).start()

    normalize(0)
    pl.semaphore_wait(bar, 2)
    for k in range(1, nk):
        normalize(k)
        send(k - 1)
    acc_qkv[near] = jnp.zeros_like(acc_qkv[near])
    send(nk - 1)
    acc_qkv[far] = jnp.zeros_like(acc_qkv[far])
    acc_up[...] = jnp.zeros_like(acc_up)

    pair = 2 * 3 * head_dim

    def up_q(k, slot, r):
        xk = xn[k, r, :]
        for h in range(0, heads, 2):
            w = jnp.concatenate([wq_buf[slot, h], wq_buf[slot, h + 1]], axis=1)
            sl = slice(h // 2 * pair, (h // 2 + 1) * pair)
            acc_qkv[r, sl] += jnp.dot(xk, w, preferred_element_type=F32)

    def up_u(k, slot, r):
        xk = xn[k, r, :]
        for n in range(0, ff, pair):
            sl = slice(n, min(n + pair, ff))
            acc_up[r, sl] += jnp.dot(xk, wu_buf[slot, :, sl], preferred_element_type=F32)

    @pl.loop(0, LOCAL_FIRST)
    def _(k):
        to_sib(k).wait_recv()
        q_copy(k, k).wait()
        up_q(k, k, near)
        u_copy(k, k).wait()
        up_u(k, k, near)

        @pl.when(k > 0)
        def _():
            to_par(k - 1).wait_recv()
            fwd(k - 1).start()

    def refill(k, slot, copy):
        @pl.when(k + U_SLOTS < nk)
        def _():
            copy(k + U_SLOTS, slot).start()

    @pl.loop(0, LOCAL_FIRST)
    def _(k):
        to_par(k + LOCAL_FIRST - 1).wait_recv()
        fwd(k + LOCAL_FIRST - 1).start()
        fwd(k).wait_recv()
        up_q(k, k, far)
        refill(k, k, q_copy)
        up_u(k, k, far)
        refill(k, k, u_copy)

    @pl.loop(LOCAL_FIRST, nk)
    def _(k):
        slot = k % U_SLOTS
        nf = k + LOCAL_FIRST - 1

        @pl.when(nf < nk)
        def _():
            to_par(nf).wait_recv()
            fwd(nf).start()

        to_sib(k).wait_recv()
        fwd(k).wait_recv()
        q_copy(k, slot).wait()
        up_q(k, slot, slice(None))
        refill(k, slot, q_copy)
        u_copy(k, slot).wait()
        up_u(k, slot, slice(None))
        refill(k, slot, u_copy)

        @pl.when(k + D_SLOTS >= nk)
        def _():
            j = k + D_SLOTS - nk
            for c in down_copies(j, j):
                c.start()

    def attention(qr):
        for h in range(heads):
            o = h * 3 * head_dim
            q = acc_qkv[qr, o:o + head_dim].astype(BF16)
            kk = acc_qkv[:, o + head_dim:o + 2 * head_dim].astype(BF16)
            vv = acc_qkv[:, o + 2 * head_dim:o + 3 * head_dim].astype(BF16)
            s = lax.dot_general(q, kk, (((1,), (1,)), ((), ())), preferred_element_type=F32) * scale
            e = jnp.exp(s - jnp.max(s, axis=-1, keepdims=True))
            l = jnp.sum(e, axis=-1, keepdims=True)
            ov = jnp.dot(e.astype(BF16), vv, preferred_element_type=F32)
            act[qr, h * head_dim:(h + 1) * head_dim] = (ov / l).astype(BF16)

    def gelu(base):
        @pl.loop(0, 2 * rows // 16)
        def _(i):
            r = pl.ds(pl.multiple_of(base + i * 16, 16), 16)
            act[r, att:] = jax.nn.gelu(acc_up[r, :], approximate=True).astype(BF16)

    def put_cross(j, p):
        snd_x[j] = p[0:rows]
        snd_sc[j] = p[rows:2 * rows]

    def put_own(j, p):
        mine[j] = p[0:rows]
        snd_so[j] = p[rows:2 * rows]

    def combine(j):
        rs_cross(j).wait_recv()
        snd_x[j] = snd_x[j] + rcv_sc[j]

    attention(far)
    gelu(2 * rows)
    for j in range(D_SLOTS):
        for c in down_copies(j, j):
            c.wait()
        put_cross(j, jnp.dot(act[far], wd_buf[j], preferred_element_type=F32))
        rs_cross(j).start()
    combine(0)
    gelu(0)
    rs_x(0).start()
    attention(near)
    for j in range(D_SLOTS):
        put_own(j, jnp.dot(act[near], wd_buf[j], preferred_element_type=F32))
        if j == 0:
            combine(1)
        rs_own(j).start()
        if j == 0:
            rs_x(1).start()
        for c in down_copies(j + D_SLOTS, j):
            c.start()

    @pl.loop(D_SLOTS, nj)
    def _(j):
        slot = j % D_SLOTS
        for c in down_copies(j, slot):
            c.wait()
        p = jnp.dot(act[...], wd_buf[slot], preferred_element_type=F32)
        put_cross(j, p[far])
        put_own(j, p[near])

        @pl.when(j > D_SLOTS)
        def _():
            combine(j - 1)

        rs_cross(j).start()
        rs_own(j).start()

        @pl.when(j > D_SLOTS)
        def _():
            rs_x(j - 1).start()

        @pl.when(j + D_SLOTS < nj)
        def _():
            for c in down_copies(j + D_SLOTS, slot):
                c.start()

    combine(nj - 1)
    rs_x(nj - 1).start()

    for j in range(nj):
        cols = slice(j * NC, (j + 1) * NC)
        rs_own(j).wait_recv()
        part = x_ref[:, cols].astype(F32) + (mine[j] + rcv_so[j])
        rs_x(j).wait_recv()
        y_ref[:, cols] = (part + rcv_x[j]).astype(BF16)

    @pl.loop(0, nk)
    def _(k):
        to_sib(k).wait_send()
        to_par(k).wait_send()
        fwd(k).wait_send()

    @pl.loop(0, nj)
    def _(j):
        rs_cross(j).wait_send()
        rs_own(j).wait_send()
        rs_x(j).wait_send()


def solution(mesh):
    def local_block(x_loc, ln_gamma, w_qkv, w_out, w_up, w_down):
        rows, dim = x_loc.shape
        heads, hd3 = w_qkv.shape[1:]
        att = heads * hd3 // 3
        ff = w_up.shape[1]
        seq = 4 * rows
        nk, nj = dim // KC, dim // NC
        vm = pl.BlockSpec(memory_space=pltpu.VMEM)
        hbm = pl.BlockSpec(memory_space=pl.ANY)
        dma = pltpu.SemaphoreType.DMA
        return pl.pallas_call(
            kernel,
            out_shape=pltpu.VMEM((rows, dim), BF16),
            in_specs=[hbm, vm, hbm, hbm, hbm, hbm],
            out_specs=vm,
            scratch_shapes=[
                pltpu.VMEM((rows, dim), BF16),
                pltpu.VMEM((2, rows, 1), F32),
                pltpu.VMEM((nk, seq, KC), BF16),
                pltpu.VMEM((seq, heads * hd3), F32),
                pltpu.VMEM((seq, ff), F32),
                pltpu.VMEM((U_SLOTS, heads, KC, hd3), BF16),
                pltpu.VMEM((U_SLOTS, KC, ff), BF16),
                pltpu.VMEM((D_SLOTS, att + ff, NC), BF16),
                pltpu.VMEM((seq, att + ff), BF16),
                pltpu.VMEM((nj, rows, NC), F32),
                pltpu.VMEM((nj, rows, NC), F32),
                pltpu.VMEM((nj, rows, NC), F32),
                pltpu.VMEM((nj, rows, NC), F32),
                pltpu.VMEM((nj, rows, NC), F32),
                pltpu.VMEM((nj, rows, NC), F32),
                pltpu.VMEM((nj, rows, NC), F32),
                dma, dma((U_SLOTS,)), dma((U_SLOTS,)), dma((D_SLOTS,)), dma((D_SLOTS,)),
                dma((nk,)), dma((nk,)), dma((nk,)), dma((nk,)), dma((nk,)), dma((nk,)),
                dma((nj,)), dma((nj,)), dma((nj,)), dma((nj,)), dma((nj,)), dma((nj,)),
            ],
            compiler_params=pltpu.CompilerParams(
                collective_id=0, has_side_effects=True, vmem_limit_bytes=66_000_000),
            cost_estimate=pl.CostEstimate(flops=32 * 10**9, bytes_accessed=125 * 10**6, transcendentals=10**6),
            name="block",
        )(x_loc, ln_gamma.reshape(1, dim), jnp.transpose(w_qkv, (1, 0, 2)), w_up,
          w_out.reshape(att, dim), w_down)

    row_spec = P(("data", "tp"), None)
    return jax.shard_map(
        local_block, mesh=mesh,
        in_specs=(row_spec, P(None), P(None, "tp", None), P("tp", None, None), P(None, "tp"), P("tp", None)),
        out_specs=row_spec, check_vma=False)
```

```python
import jax
import jax.numpy as jnp
from jax import lax
from jax.experimental import pallas as pl
from jax.experimental.pallas import tpu as pltpu
from jax.sharding import PartitionSpec as P

LN_EPS = 1e-6
MESH = pl.DeviceIdType.MESH
F32 = jnp.float32
BF16 = jnp.bfloat16

KC = 512
NC = 384
SLOTS = 5
SPLIT = 3
LATE = 2


def kernel(x_hbm, g_hbm, wqkv_ref, wup_ref, wout_ref, wdown_ref, y_ref,
           x_ref, g_ref, stat, xn, acc_qkv, acc_up, wq_buf, wu_buf, act,
           snd_sc, rcv_sc, snd_so, rcv_so, snd_x, rcv_x, mine,
           sem_in, sem_g, sem_wq, sem_wu, sem_wo, sem_wd,
           s_sib, r_sib, s_par, r_par, s_fwd, r_fwd,
           s_rc, r_rc, s_ro, r_ro, s_rx, r_rx):
    rows, dim = x_ref.shape
    heads, head_dim = wout_ref.shape[:2]
    ff = wup_ref.shape[1]
    att = heads * head_dim
    nk, nj = dim // KC, pl.cdiv(dim, NC)
    ksub, n_out = KC // head_dim, (att + ff) // head_dim
    d = lax.axis_index("data")
    t = lax.axis_index("tp")
    sib = (d, t + 1 - 2 * (t % 2))
    par = (d, (t + 2) % 4)
    scale = head_dim ** -0.5
    near, far = slice(0, 2 * rows), slice(2 * rows, 4 * rows)

    x_in = pltpu.make_async_copy(x_hbm, x_ref, sem_in)
    x_in.start()
    g_in = pltpu.make_async_copy(g_hbm, g_ref, sem_g)
    g_in.start()

    bar = pltpu.get_barrier_semaphore()
    for peer in (sib, par):
        pl.semaphore_signal(bar, inc=1, device_id=peer, device_id_type=MESH)

    def q_copies(k, slot):
        return [pltpu.make_async_copy(
            wqkv_ref.at[h, pl.ds(k * ksub, ksub)], wq_buf.at[slot, pl.ds(h * ksub, ksub)], sem_wq.at[slot, h])
            for h in range(heads)]

    def u_copy(k, slot):
        return pltpu.make_async_copy(wup_ref.at[pl.ds(k * KC, KC), :], wu_buf.at[slot], sem_wu.at[slot])

    def down_copies(j, slot, n=NC):
        src, dst = pl.ds(j * NC, n), pl.ds(0, n)
        return (
            pltpu.make_async_copy(wout_ref.at[:, :, src], wq_buf.at[slot, pl.ds(0, heads), :, dst], sem_wo.at[slot]),
            pltpu.make_async_copy(
                wdown_ref.at[:, :, src], wq_buf.at[slot, pl.ds(heads, n_out - heads), :, dst], sem_wd.at[slot]),
        )

    def remote(src, dst, ssem, rsem, peer):
        return pltpu.make_async_remote_copy(
            src_ref=src, dst_ref=dst, send_sem=ssem, recv_sem=rsem,
            device_id=peer, device_id_type=MESH)

    def blk(r):
        return pl.ds(r * rows, rows)

    def to_sib(k):
        return remote(xn.at[k, blk(0), :], xn.at[k, blk(1), :], s_sib.at[k], r_sib.at[k], sib)

    def to_par(k):
        return remote(xn.at[k, blk(0), :], xn.at[k, blk(2), :], s_par.at[k], r_par.at[k], par)

    def fwd(k):
        return remote(xn.at[k, blk(2), :], xn.at[k, blk(3), :], s_fwd.at[k], r_fwd.at[k], sib)

    def rs_cross(j, n=NC):
        c = pl.ds(0, n)
        return remote(snd_sc.at[j, :, c], rcv_sc.at[j, :, c], s_rc.at[j], r_rc.at[j], sib)

    def rs_own(j, n=NC):
        c = pl.ds(0, n)
        return remote(snd_so.at[j, :, c], rcv_so.at[j, :, c], s_ro.at[j], r_ro.at[j], sib)

    def rs_x(j, n=NC):
        c = pl.ds(0, n)
        return remote(snd_x.at[j, :, c], rcv_x.at[j, :, c], s_rx.at[j], r_rx.at[j], par)

    def start_up(k, slot):
        for c in q_copies(k, slot) + [u_copy(k, slot)]:
            c.start()

    start_up(0, 0)

    x_in.wait()
    for i in range(rows // 16):
        r = slice(i * 16, (i + 1) * 16)
        v = x_ref[r, :].astype(F32)
        mean = jnp.mean(v, axis=-1, keepdims=True)
        cen = v - mean
        var = jnp.mean(cen * cen, axis=-1, keepdims=True)
        stat[0, r, :] = mean
        stat[1, r, :] = lax.rsqrt(var + LN_EPS)

    start_up(1, 1)

    def normalize(k):
        c = slice(k * KC, (k + 1) * KC)
        cen = x_ref[:, c].astype(F32) - stat[0]
        xn[k, 0:rows, :] = (cen * stat[1] * g_ref[:, c]).astype(BF16)

    def send(k):
        to_par(k).start()
        to_sib(k).start()

    g_in.wait()
    normalize(0)
    pl.semaphore_wait(bar, 2)
    start_up(2, 2)
    for k in range(1, nk):
        normalize(k)
        send(k - 1)
    acc_qkv[near] = jnp.zeros_like(acc_qkv[near])
    send(nk - 1)
    acc_qkv[far] = jnp.zeros_like(acc_qkv[far])
    acc_up[...] = jnp.zeros_like(acc_up)

    pair = 2 * 3 * head_dim

    def q_pass(k, slot, r):
        xk = xn[k, r, :]
        for h in range(0, heads, 2):
            w = jnp.concatenate(
                [wq_buf[slot, i * ksub:(i + 1) * ksub].reshape(KC, 3 * head_dim) for i in (h, h + 1)], axis=1)
            sl = slice(h // 2 * pair, (h // 2 + 1) * pair)
            acc_qkv[r, sl] += jnp.dot(xk, w, preferred_element_type=F32)

    def u_pass(k, slot, r, final=False):
        xk = xn[k, r, :]
        for n in range(0, ff, pair):
            end = min(n + pair, ff)
            total = acc_up[r, n:end] + jnp.dot(xk, wu_buf[slot, :, n:end], preferred_element_type=F32)
            if final:
                act[r, att + n:att + end] = jax.nn.gelu(total, approximate=True).astype(BF16)
            else:
                acc_up[r, n:end] = total

    def start_q(k, slot):
        for c in q_copies(k, slot):
            c.start()

    def wait_q(k, slot):
        for c in q_copies(k, slot):
            c.wait()

    def start_down(j, slot, n=NC):
        for c in down_copies(j, slot, n):
            c.start()

    def forward(k):
        to_par(k).wait_recv()
        fwd(k).start()

    early = nk - LATE - SLOTS

    def refill(f, slot):
        start_q(f + SLOTS, slot)

        @pl.when(f < early)
        def _():
            u_copy(f + SLOTS, slot).start()

        @pl.when(f == SLOTS - 1)
        def _():
            for i in range(early, SLOTS):
                u_copy(i + SLOTS, i).start()

    @pl.loop(0, SPLIT + 1)
    def _(k):
        @pl.when(k < SPLIT)
        def _():
            to_sib(k).wait_recv()
            wait_q(k, k)
            u_copy(k, k).wait()

            @pl.when(k + SPLIT < SLOTS)
            def _():
                start_up(k + SPLIT, k + SPLIT)

            q_pass(k, k, near)
            u_pass(k, k, near)

        forward(k)

        @pl.when(k > 0)
        def _():
            f = k - 1
            fwd(f).wait_recv()
            q_pass(f, f, far)
            u_pass(f, f, far)
            refill(f, f)

    def full_waits(k, slot):
        @pl.when(k + 1 < nk)
        def _():
            forward(k + 1)

        to_sib(k).wait_recv()
        fwd(k).wait_recv()
        wait_q(k, slot)

    @pl.loop(SPLIT, SLOTS)
    def _(k):
        full_waits(k, k)
        u_copy(k, k).wait()
        q_pass(k, k, slice(None))
        u_pass(k, k, slice(None))
        refill(k, k)

    @pl.loop(SLOTS, nk - LATE)
    def _(k):
        slot = k - SLOTS
        full_waits(k, slot)
        u_copy(k, slot).wait()
        q_pass(k, slot, slice(None))
        u_pass(k, slot, far)
        start_down(slot, slot)

    @pl.loop(nk - LATE, nk)
    def _(k):
        slot = k - SLOTS
        full_waits(k, slot)
        q_pass(k, slot, slice(None))
        start_down(slot, slot)

    def attention(qr):
        for h in range(heads):
            o = h * 3 * head_dim
            q = acc_qkv[qr, o:o + head_dim].astype(BF16)
            kk = acc_qkv[:, o + head_dim:o + 2 * head_dim].astype(BF16)
            vv = acc_qkv[:, o + 2 * head_dim:o + 3 * head_dim].astype(BF16)
            s = lax.dot_general(q, kk, (((1,), (1,)), ((), ())), preferred_element_type=F32) * scale
            e = jnp.exp(s - jnp.max(s, axis=-1, keepdims=True))
            l = jnp.sum(e, axis=-1, keepdims=True)
            ov = jnp.dot(e.astype(BF16), vv, preferred_element_type=F32)
            act[qr, h * head_dim:(h + 1) * head_dim] = (ov / l).astype(BF16)

    last, n_last = nj - 1, dim - (nj - 1) * NC

    def product(slot, r, n):
        w = wq_buf[slot, 0:n_out, :, 0:n].reshape(att + ff, n)
        return jnp.dot(act[r], w, preferred_element_type=F32)

    def cross(j, slot, n=NC):
        p = product(slot, far, n)
        snd_x[j, :, 0:n] = p[0:rows]
        snd_sc[j, :, 0:n] = p[rows:2 * rows]
        rs_cross(j, n).start()

    def own(j, slot, n=NC):
        p = product(slot, near, n)
        mine[j, :, 0:n] = p[0:rows]
        snd_so[j, :, 0:n] = p[rows:2 * rows]
        rs_own(j, n).start()

    def combine(j, n=NC):
        rs_cross(j, n).wait_recv()
        snd_x[j, :, 0:n] = snd_x[j, :, 0:n] + rcv_sc[j, :, 0:n]
        rs_x(j, n).start()

    def wait_down(j, slot, n=NC):
        for c in down_copies(j, slot, n):
            c.wait()

    for i in range(early, SLOTS):
        u_copy(i + SLOTS, i).wait()
    for i in range(early, SLOTS):
        u_pass(i + SLOTS, i, far, i == SLOTS - 1)
    attention(far)

    @pl.loop(0, 3)
    def _(j):
        wait_down(j, j)
        cross(j, j)

        @pl.loop(jnp.maximum(2 * j - 1, 0), jnp.minimum(2 * j + 1, SLOTS - 1))
        def _(i):
            u_pass(i + SLOTS, i, near)

        combine(j)

    wait_down(3, 3)
    cross(3, 3)
    u_pass(nk - 1, SLOTS - 1, near, True)
    attention(near)
    combine(3)

    def refill_down(j):
        slot = j % SLOTS

        @pl.when(j + SLOTS < last)
        def _():
            start_down(j + SLOTS, slot)

        @pl.when(j + SLOTS == last)
        def _():
            start_down(last, slot, n_last)

    own(0, 0)
    refill_down(0)

    @pl.loop(4, last)
    def _(j):
        wait_down(j, j % SLOTS)
        cross(j, j % SLOTS)
        o = jnp.where(j == 4, 1, j - 2)
        own(o, o % SLOTS)
        combine(j)
        refill_down(o)

        @pl.when(j == 4)
        def _():
            own(2, 2)
            refill_down(2)

    wait_down(last, last % SLOTS, n_last)
    cross(last, last % SLOTS, n_last)
    own(last - 2, (last - 2) % SLOTS)
    combine(last, n_last)
    own(last - 1, (last - 1) % SLOTS)
    own(last, last % SLOTS, n_last)

    for j in range(nj):
        n = n_last if j == last else NC
        cols = slice(j * NC, j * NC + n)
        rs_own(j, n).wait_recv()
        part = x_ref[:, cols].astype(F32) + (mine[j, :, 0:n] + rcv_so[j, :, 0:n])
        rs_x(j, n).wait_recv()
        y_ref[:, cols] = (part + rcv_x[j, :, 0:n]).astype(BF16)

    @pl.loop(0, nk)
    def _(k):
        to_sib(k).wait_send()
        to_par(k).wait_send()
        fwd(k).wait_send()

    for j in range(nj):
        n = n_last if j == last else NC
        rs_cross(j, n).wait_send()
        rs_own(j, n).wait_send()
        rs_x(j, n).wait_send()


def solution(mesh):
    def local_block(x_loc, ln_gamma, w_qkv, w_out, w_up, w_down):
        rows, dim = x_loc.shape
        heads, hd3 = w_qkv.shape[1:]
        hd = hd3 // 3
        att = heads * hd
        ff = w_up.shape[1]
        seq = 4 * rows
        nk, nj = dim // KC, pl.cdiv(dim, NC)
        vm = pl.BlockSpec(memory_space=pltpu.VMEM)
        hbm = pl.BlockSpec(memory_space=pl.ANY)
        dma = pltpu.SemaphoreType.DMA
        return pl.pallas_call(
            kernel,
            out_shape=pltpu.VMEM((rows, dim), BF16),
            in_specs=[hbm, hbm, hbm, hbm, hbm, hbm],
            out_specs=vm,
            scratch_shapes=[
                pltpu.VMEM((rows, dim), BF16),
                pltpu.VMEM((1, dim), F32),
                pltpu.VMEM((2, rows, 1), F32),
                pltpu.VMEM((nk, seq, KC), BF16),
                pltpu.VMEM((seq, heads * hd3), F32),
                pltpu.VMEM((seq, ff), F32),
                pltpu.VMEM((SLOTS, heads * KC // hd, hd, hd3), BF16),
                pltpu.VMEM((SLOTS, KC, ff), BF16),
                pltpu.VMEM((seq, att + ff), BF16),
                pltpu.VMEM((nj, rows, NC), F32),
                pltpu.VMEM((nj, rows, NC), F32),
                pltpu.VMEM((nj, rows, NC), F32),
                pltpu.VMEM((nj, rows, NC), F32),
                pltpu.VMEM((nj, rows, NC), F32),
                pltpu.VMEM((nj, rows, NC), F32),
                pltpu.VMEM((nj, rows, NC), F32),
                dma, dma, dma((SLOTS, heads)), dma((SLOTS,)), dma((SLOTS,)), dma((SLOTS,)),
                dma((nk,)), dma((nk,)), dma((nk,)), dma((nk,)), dma((nk,)), dma((nk,)),
                dma((nj,)), dma((nj,)), dma((nj,)), dma((nj,)), dma((nj,)), dma((nj,)),
            ],
            compiler_params=pltpu.CompilerParams(
                collective_id=0, has_side_effects=True, vmem_limit_bytes=66_000_000),
            cost_estimate=pl.CostEstimate(flops=32 * 10**9, bytes_accessed=125 * 10**6, transcendentals=10**6),
            name="block",
        )(x_loc, ln_gamma.reshape(1, dim), jnp.transpose(w_qkv, (1, 0, 2)).reshape(heads, dim // hd, hd, hd3), w_up,
          w_out, w_down.reshape(ff // hd, hd, dim))

    row_spec = P(("data", "tp"), None)
    return jax.shard_map(
        local_block, mesh=mesh,
        in_specs=(row_spec, P(None), P(None, "tp", None), P("tp", None, None), P(None, "tp"), P("tp", None)),
        out_specs=row_spec, check_vma=False)
```

```python
import jax
import jax.numpy as jnp
from jax import lax
from jax.experimental import pallas as pl
from jax.experimental.pallas import tpu as pltpu
from jax.sharding import PartitionSpec as P

LN_EPS = 1e-6
MESH = pl.DeviceIdType.MESH
F32 = jnp.float32
BF16 = jnp.bfloat16

KC = 512
NC = 384
SLOTS = 5


def kernel(x_hbm, g_hbm, wqkv_ref, wup_ref, wout_ref, wdown_ref, y_ref,
           x_ref, g_ref, stat, xn, acc_qkv, acc_up, wq_buf, wu_buf, act,
           snd_sc, rcv_sc, snd_so, rcv_so, snd_x, rcv_x, mine,
           sem_in, sem_g, sem_wq, sem_wu, sem_wo, sem_wd,
           s_sib, r_sib, s_par, r_par, s_fwd, r_fwd,
           s_rc, r_rc, s_ro, r_ro, s_rx, r_rx):
    rows, dim = x_ref.shape
    heads, head_dim = wout_ref.shape[:2]
    ff = wup_ref.shape[1]
    att = heads * head_dim
    nk, nj = dim // KC, pl.cdiv(dim, NC)
    ksub, n_out = KC // head_dim, (att + ff) // head_dim
    d = lax.axis_index("data")
    t = lax.axis_index("tp")
    sib = (d, t + 1 - 2 * (t % 2))
    par = (d, (t + 2) % 4)
    scale = head_dim ** -0.5
    near, far = slice(0, 2 * rows), slice(2 * rows, 4 * rows)

    x_in = pltpu.make_async_copy(x_hbm, x_ref, sem_in)
    x_in.start()
    g_in = pltpu.make_async_copy(g_hbm, g_ref, sem_g)
    g_in.start()

    bar = pltpu.get_barrier_semaphore()
    for peer in (sib, par):
        pl.semaphore_signal(bar, inc=1, device_id=peer, device_id_type=MESH)

    def q_copies(k, slot):
        return [pltpu.make_async_copy(
            wqkv_ref.at[h, pl.ds(k * ksub, ksub)], wq_buf.at[slot, pl.ds(h * ksub, ksub)], sem_wq.at[slot, h])
            for h in range(heads)]

    def u_copy(k, slot):
        return pltpu.make_async_copy(wup_ref.at[pl.ds(k * KC, KC), :], wu_buf.at[slot], sem_wu.at[slot])

    def down_copies(j, slot, n=NC):
        src, dst = pl.ds(j * NC, n), pl.ds(0, n)
        return (
            pltpu.make_async_copy(wout_ref.at[:, :, src], wq_buf.at[slot, pl.ds(0, heads), :, dst], sem_wo.at[slot]),
            pltpu.make_async_copy(
                wdown_ref.at[:, :, src], wq_buf.at[slot, pl.ds(heads, n_out - heads), :, dst], sem_wd.at[slot]),
        )

    def remote(src, dst, ssem, rsem, peer):
        return pltpu.make_async_remote_copy(
            src_ref=src, dst_ref=dst, send_sem=ssem, recv_sem=rsem,
            device_id=peer, device_id_type=MESH)

    def blk(r):
        return pl.ds(r * rows, rows)

    def to_sib(k):
        return remote(xn.at[k, blk(0), :], xn.at[k, blk(1), :], s_sib.at[k], r_sib.at[k], sib)

    def to_par(k):
        return remote(xn.at[k, blk(0), :], xn.at[k, blk(2), :], s_par.at[k], r_par.at[k], par)

    def fwd(k):
        return remote(xn.at[k, blk(2), :], xn.at[k, blk(3), :], s_fwd.at[k], r_fwd.at[k], sib)

    def rs_cross(j, n=NC):
        c = pl.ds(0, n)
        return remote(snd_sc.at[j, :, c], rcv_sc.at[j, :, c], s_rc.at[j], r_rc.at[j], sib)

    def rs_own(j, n=NC):
        c = pl.ds(0, n)
        return remote(snd_so.at[j, :, c], rcv_so.at[j, :, c], s_ro.at[j], r_ro.at[j], sib)

    def rs_x(j, n=NC):
        c = pl.ds(0, n)
        return remote(snd_x.at[j, :, c], rcv_x.at[j, :, c], s_rx.at[j], r_rx.at[j], par)

    def start_up(k, slot):
        for c in q_copies(k, slot) + [u_copy(k, slot)]:
            c.start()

    start_up(0, 0)

    x_in.wait()
    for i in range(rows // 16):
        r = slice(i * 16, (i + 1) * 16)
        v = x_ref[r, :].astype(F32)
        mean = jnp.mean(v, axis=-1, keepdims=True)
        cen = v - mean
        var = jnp.mean(cen * cen, axis=-1, keepdims=True)
        stat[0, r, :] = mean
        stat[1, r, :] = lax.rsqrt(var + LN_EPS)

    start_up(1, 1)

    def normalize(k):
        c = slice(k * KC, (k + 1) * KC)
        cen = x_ref[:, c].astype(F32) - stat[0]
        xn[k, 0:rows, :] = (cen * stat[1] * g_ref[:, c]).astype(BF16)

    def send(k):
        to_par(k).start()
        to_sib(k).start()

    g_in.wait()
    normalize(0)
    pl.semaphore_wait(bar, 2)
    start_up(2, 2)
    for k in range(1, nk):
        normalize(k)
        send(k - 1)
    acc_qkv[near] = jnp.zeros_like(acc_qkv[near])
    send(nk - 1)
    acc_qkv[far] = jnp.zeros_like(acc_qkv[far])
    acc_up[...] = jnp.zeros_like(acc_up)

    pair = 2 * 3 * head_dim

    def ksum(terms):
        return sum(jnp.dot(x, w, preferred_element_type=F32) for x, w in terms)

    def q_pass(ks, r):
        for h in range(0, heads, 2):
            sl = slice(h // 2 * pair, (h // 2 + 1) * pair)
            acc_qkv[r, sl] += ksum(
                (xn[k, r, :], jnp.concatenate(
                    [wq_buf[slot, i * ksub:(i + 1) * ksub].reshape(KC, 3 * head_dim) for i in (h, h + 1)], axis=1))
                for k, slot in ks)

    def u_pass(ks, r, final=False):
        for n in range(0, ff, pair):
            end = min(n + pair, ff)
            total = acc_up[r, n:end] + ksum((xn[k, r, :], wu_buf[slot, :, n:end]) for k, slot in ks)
            if final:
                act[r, att + n:att + end] = jax.nn.gelu(total, approximate=True).astype(BF16)
            else:
                acc_up[r, n:end] = total

    def start_q(k, slot):
        for c in q_copies(k, slot):
            c.start()

    def wait_q(k, slot):
        for c in q_copies(k, slot):
            c.wait()

    def start_down(j, slot, n=NC):
        for c in down_copies(j, slot, n):
            c.start()

    def forward(k):
        to_par(k).wait_recv()
        fwd(k).start()

    everyone = slice(None)

    def next_q(k):
        start_q(k + SLOTS, k)

    def next_u(k):
        u_copy(k + SLOTS, k).start()

    def wait_rows(k):
        to_sib(k).wait_recv()
        fwd(k).wait_recv()

    @pl.loop(0, 3)
    def _(k):
        to_sib(k).wait_recv()
        wait_q(k, k)
        u_copy(k, k).wait()

        @pl.when(k + 3 < SLOTS)
        def _():
            start_up(k + 3, k + 3)

        q_pass([(k, k)], near)
        u_pass([(k, k)], near)
        forward(k + k // 2)

        @pl.when(k == 1)
        def _():
            fwd(0).wait_recv()
            q_pass([(0, 0)], far)
            u_pass([(0, 0)], far)
            next_q(0)
            next_u(0)
            forward(2)

    fwd(1).wait_recv()
    fwd(2).wait_recv()
    q_pass([(1, 1), (2, 2)], far)
    u_pass([(1, 1), (2, 2)], far)
    next_q(1)
    next_u(1)
    next_q(2)
    next_u(2)
    forward(4)

    @pl.loop(3, SLOTS)
    def _(k):
        wait_rows(k)
        wait_q(k, k)
        u_copy(k, k).wait()
        q_pass([(k, k)], everyone)
        u_pass([(k, k)], everyone)
        next_q(k)

        @pl.when(k == 4)
        def _():
            next_u(3)
            next_u(4)

        forward(2 * k - 1)
        forward(2 * k)

    for k in (5, 6):
        wait_rows(k)
        wait_q(k, k - SLOTS)
        u_copy(k, k - SLOTS).wait()
    q_pass([(5, 0), (6, 1)], everyone)
    u_pass([(5, 0), (6, 1)], far)
    start_down(0, 0)
    start_down(1, 1)
    forward(9)
    for k in (7, 8):
        wait_rows(k)
        wait_q(k, k - SLOTS)
    u_copy(7, 2).wait()
    q_pass([(7, 2), (8, 3)], everyone)
    u_pass([(7, 2)], far)
    start_down(2, 2)
    start_down(3, 3)
    wait_rows(9)
    wait_q(9, 4)
    u_copy(8, 3).wait()
    u_copy(9, 4).wait()
    q_pass([(9, 4)], everyone)

    def attention(qr):
        for h in range(heads):
            o = h * 3 * head_dim
            q = acc_qkv[qr, o:o + head_dim].astype(BF16)
            kk = acc_qkv[:, o + head_dim:o + 2 * head_dim].astype(BF16)
            vv = acc_qkv[:, o + 2 * head_dim:o + 3 * head_dim].astype(BF16)
            s = lax.dot_general(q, kk, (((1,), (1,)), ((), ())), preferred_element_type=F32) * scale
            e = jnp.exp(s - jnp.max(s, axis=-1, keepdims=True))
            l = jnp.sum(e, axis=-1, keepdims=True)
            ov = jnp.dot(e.astype(BF16), vv, preferred_element_type=F32)
            act[qr, h * head_dim:(h + 1) * head_dim] = (ov / l).astype(BF16)

    last, n_last = nj - 1, dim - (nj - 1) * NC

    def product(slot, r, n):
        w = wq_buf[slot, 0:n_out, :, 0:n].reshape(att + ff, n)
        return jnp.dot(act[r], w, preferred_element_type=F32)

    def cross(j, slot, n=NC):
        p = product(slot, far, n)
        snd_x[j, :, 0:n] = p[0:rows]
        snd_sc[j, :, 0:n] = p[rows:2 * rows]
        rs_cross(j, n).start()

    def own(j, slot, n=NC):
        p = product(slot, near, n)
        mine[j, :, 0:n] = p[0:rows]
        snd_so[j, :, 0:n] = p[rows:2 * rows]
        rs_own(j, n).start()

    def combine(j, n=NC):
        rs_cross(j, n).wait_recv()
        snd_x[j, :, 0:n] = snd_x[j, :, 0:n] + rcv_sc[j, :, 0:n]
        rs_x(j, n).start()

    def wait_down(j, slot, n=NC):
        for c in down_copies(j, slot, n):
            c.wait()

    u_pass([(8, 3), (9, 4)], far, True)
    attention(far)
    start_down(4, 4)

    wait_down(0, 0)
    cross(0, 0)
    u_pass([(5, 0), (6, 1)], near)
    combine(0)
    wait_down(1, 1)
    cross(1, 1)
    u_pass([(7, 2), (8, 3)], near)
    combine(1)
    wait_down(2, 2)
    cross(2, 2)
    u_pass([(9, 4)], near, True)
    attention(near)
    combine(2)

    def refill_down(j):
        slot = j % SLOTS

        @pl.when(j + SLOTS < last)
        def _():
            start_down(j + SLOTS, slot)

        @pl.when(j + SLOTS == last)
        def _():
            start_down(last, slot, n_last)

    wait_down(3, 3)
    cross(3, 3)
    own(0, 0)
    combine(3)
    refill_down(0)

    @pl.loop(4, last)
    def _(j):
        wait_down(j, j % SLOTS)
        cross(j, j % SLOTS)
        own(j - 3, (j - 3) % SLOTS)
        combine(j)
        refill_down(j - 3)

    wait_down(last, last % SLOTS, n_last)
    cross(last, last % SLOTS, n_last)
    own(last - 3, (last - 3) % SLOTS)
    combine(last, n_last)

    @pl.loop(last - 2, last)
    def _(j):
        own(j, j % SLOTS)

    own(last, last % SLOTS, n_last)

    @pl.loop(0, nk)
    def _(k):
        to_sib(k).wait_send()
        to_par(k).wait_send()
        fwd(k).wait_send()

    @pl.loop(0, last)
    def _(j):
        rs_cross(j).wait_send()
        rs_own(j).wait_send()

    @pl.loop(0, last - 2)
    def _(j):
        rs_x(j).wait_send()

    rs_cross(last, n_last).wait_send()
    rs_own(last, n_last).wait_send()

    for j in range(nj):
        n = n_last if j == last else NC
        cols = slice(j * NC, j * NC + n)
        rs_own(j, n).wait_recv()
        part = x_ref[:, cols].astype(F32) + (mine[j, :, 0:n] + rcv_so[j, :, 0:n])
        rs_x(j, n).wait_recv()
        y_ref[:, cols] = (part + rcv_x[j, :, 0:n]).astype(BF16)

    rs_x(last - 2).wait_send()
    rs_x(last - 1).wait_send()
    rs_x(last, n_last).wait_send()


def solution(mesh):
    def local_block(x_loc, ln_gamma, w_qkv, w_out, w_up, w_down):
        rows, dim = x_loc.shape
        heads, hd3 = w_qkv.shape[1:]
        hd = hd3 // 3
        att = heads * hd
        ff = w_up.shape[1]
        seq = 4 * rows
        nk, nj = dim // KC, pl.cdiv(dim, NC)
        vm = pl.BlockSpec(memory_space=pltpu.VMEM)
        hbm = pl.BlockSpec(memory_space=pl.ANY)
        dma = pltpu.SemaphoreType.DMA
        return pl.pallas_call(
            kernel,
            out_shape=pltpu.VMEM((rows, dim), BF16),
            in_specs=[hbm, hbm, hbm, hbm, hbm, hbm],
            out_specs=vm,
            scratch_shapes=[
                pltpu.VMEM((rows, dim), BF16),
                pltpu.VMEM((1, dim), F32),
                pltpu.VMEM((2, rows, 1), F32),
                pltpu.VMEM((nk, seq, KC), BF16),
                pltpu.VMEM((seq, heads * hd3), F32),
                pltpu.VMEM((seq, ff), F32),
                pltpu.VMEM((SLOTS, heads * KC // hd, hd, hd3), BF16),
                pltpu.VMEM((SLOTS, KC, ff), BF16),
                pltpu.VMEM((seq, att + ff), BF16),
                pltpu.VMEM((nj, rows, NC), F32),
                pltpu.VMEM((nj, rows, NC), F32),
                pltpu.VMEM((nj, rows, NC), F32),
                pltpu.VMEM((nj, rows, NC), F32),
                pltpu.VMEM((nj, rows, NC), F32),
                pltpu.VMEM((nj, rows, NC), F32),
                pltpu.VMEM((nj, rows, NC), F32),
                dma, dma, dma((SLOTS, heads)), dma((SLOTS,)), dma((SLOTS,)), dma((SLOTS,)),
                dma((nk,)), dma((nk,)), dma((nk,)), dma((nk,)), dma((nk,)), dma((nk,)),
                dma((nj,)), dma((nj,)), dma((nj,)), dma((nj,)), dma((nj,)), dma((nj,)),
            ],
            compiler_params=pltpu.CompilerParams(
                collective_id=0, has_side_effects=True, vmem_limit_bytes=66_000_000),
            cost_estimate=pl.CostEstimate(flops=32 * 10**9, bytes_accessed=125 * 10**6, transcendentals=10**6),
            name="block",
        )(x_loc, ln_gamma.reshape(1, dim), jnp.transpose(w_qkv, (1, 0, 2)).reshape(heads, dim // hd, hd, hd3), w_up,
          w_out, w_down.reshape(ff // hd, hd, dim))

    row_spec = P(("data", "tp"), None)
    return jax.shard_map(
        local_block, mesh=mesh,
        in_specs=(row_spec, P(None), P(None, "tp", None), P("tp", None, None), P(None, "tp"), P("tp", None)),
        out_specs=row_spec, check_vma=False)
```

```python
import jax
import jax.numpy as jnp
from jax import lax
from jax.experimental import pallas as pl
from jax.experimental.pallas import tpu as pltpu
from jax.sharding import PartitionSpec as P

LN_EPS = 1e-6
MESH = pl.DeviceIdType.MESH
F32 = jnp.float32
BF16 = jnp.bfloat16

KC = 512
NC = 384
SLOTS = 5


def kernel(x_hbm, g_hbm, wqkv_ref, wup_ref, wout_ref, wdown_ref, y_ref,
           x_ref, g_ref, stat, xn, acc_qkv, acc_up, wq_buf, wu_buf, act,
           snd_sc, rcv_sc, snd_so, rcv_so, snd_x, rcv_x, mine,
           sem_in, sem_g, sem_wq, sem_wu, sem_wd,
           s_sib, r_sib, s_par, r_par, s_fwd, r_fwd,
           s_rc, r_rc, s_ro, r_ro, s_rx, r_rx):
    rows, dim = x_ref.shape
    heads, head_dim = wout_ref.shape[:2]
    ff = wup_ref.shape[1]
    att = heads * head_dim
    nk, nj = dim // KC, pl.cdiv(dim, NC)
    last, n_last = nj - 1, dim - (nj - 1) * NC
    ksub, n_out = KC // head_dim, (att + ff) // head_dim
    d = lax.axis_index("data")
    t = lax.axis_index("tp")
    sib = (d, t + 1 - 2 * (t % 2))
    par = (d, (t + 2) % 4)
    scale = head_dim ** -0.5
    near, far = slice(0, 2 * rows), slice(2 * rows, 4 * rows)

    x_in = pltpu.make_async_copy(x_hbm, x_ref, sem_in)
    x_in.start()
    g_in = pltpu.make_async_copy(g_hbm, g_ref, sem_g)
    g_in.start()

    bar = pltpu.get_barrier_semaphore()
    for peer in (sib, par):
        pl.semaphore_signal(bar, inc=1, device_id=peer, device_id_type=MESH)

    def q_copies(k, slot):
        return [pltpu.make_async_copy(
            wqkv_ref.at[h, pl.ds(k * ksub, ksub)], wq_buf.at[slot, pl.ds(h * ksub, ksub)], sem_wq.at[slot])
            for h in range(heads)]

    def u_copy(k, slot):
        return pltpu.make_async_copy(wup_ref.at[pl.ds(k * KC, KC), :], wu_buf.at[slot], sem_wu.at[slot])

    def down_copies(j, slot, n=NC):
        src, dst = pl.ds(j * NC, n), pl.ds(0, n)
        return (
            pltpu.make_async_copy(wout_ref.at[:, :, src], wq_buf.at[slot, pl.ds(0, heads), :, dst], sem_wd.at[slot]),
            pltpu.make_async_copy(
                wdown_ref.at[:, :, src], wq_buf.at[slot, pl.ds(heads, n_out - heads), :, dst], sem_wd.at[slot]),
        )

    def remote(src, dst, ssem, rsem, peer):
        return pltpu.make_async_remote_copy(
            src_ref=src, dst_ref=dst, send_sem=ssem, recv_sem=rsem,
            device_id=peer, device_id_type=MESH)

    def blk(r):
        return pl.ds(r * rows, rows)

    def to_sib(k):
        return remote(xn.at[k, blk(0), :], xn.at[k, blk(1), :], s_sib, r_sib.at[k], sib)

    def to_par(k):
        return remote(xn.at[k, blk(0), :], xn.at[k, blk(2), :], s_par, r_par.at[k], par)

    def fwd(k):
        return remote(xn.at[k, blk(2), :], xn.at[k, blk(3), :], s_fwd, r_fwd.at[k], sib)

    def rs_cross(j, n=NC):
        c = pl.ds(0, n)
        return remote(snd_sc.at[j, :, c], rcv_sc.at[j, :, c], s_rc.at[j // last], r_rc.at[j], sib)

    def rs_own(j, n=NC):
        c = pl.ds(0, n)
        return remote(snd_so.at[j, :, c], rcv_so.at[j, :, c], s_ro.at[j // last], r_ro.at[j // last], sib)

    def rs_x(j, n=NC):
        c = pl.ds(0, n)
        return remote(snd_x.at[j, :, c], rcv_x.at[j, :, c], s_rx.at[j // last], r_rx.at[j], par)

    def start_up(k, slot):
        for c in q_copies(k, slot) + [u_copy(k, slot)]:
            c.start()

    start_up(0, 0)

    x_in.wait()
    for i in range(rows // 16):
        r = slice(i * 16, (i + 1) * 16)
        v = x_ref[r, :].astype(F32)
        mean = jnp.mean(v, axis=-1, keepdims=True)
        cen = v - mean
        var = jnp.mean(cen * cen, axis=-1, keepdims=True)
        stat[0, r, :] = mean
        stat[1, r, :] = lax.rsqrt(var + LN_EPS)

    start_up(1, 1)

    def normalize(k):
        c = slice(k * KC, (k + 1) * KC)
        cen = x_ref[:, c].astype(F32) - stat[0]
        xn[k, 0:rows, :] = (cen * stat[1] * g_ref[:, c]).astype(BF16)

    def send(k):
        to_par(k).start()
        to_sib(k).start()

    g_in.wait()
    normalize(0)
    pl.semaphore_wait(bar, 2)
    start_up(2, 2)
    for k in range(1, nk):
        normalize(k)
        send(k - 1)
    acc_qkv[near] = jnp.zeros_like(acc_qkv[near])
    send(nk - 1)
    acc_qkv[far] = jnp.zeros_like(acc_qkv[far])
    acc_up[...] = jnp.zeros_like(acc_up)

    pair = 2 * 3 * head_dim

    def ksum(terms):
        return sum(jnp.dot(x, w, preferred_element_type=F32) for x, w in terms)

    def q_pass(ks, r):
        for h in range(0, heads, 2):
            sl = slice(h // 2 * pair, (h // 2 + 1) * pair)
            acc_qkv[r, sl] += ksum(
                (xn[k, r, :], jnp.concatenate(
                    [wq_buf[slot, i * ksub:(i + 1) * ksub].reshape(KC, 3 * head_dim) for i in (h, h + 1)], axis=1))
                for k, slot in ks)

    def u_pass(ks, r, final=False):
        for n in range(0, ff, pair):
            end = min(n + pair, ff)
            total = acc_up[r, n:end] + ksum((xn[k, r, :], wu_buf[slot, :, n:end]) for k, slot in ks)
            if final:
                act[r, att + n:att + end] = jax.nn.gelu(total, approximate=True).astype(BF16)
            else:
                acc_up[r, n:end] = total

    def start_q(k, slot):
        for c in q_copies(k, slot):
            c.start()

    def wait_q(k, slot):
        pltpu.make_async_copy(wq_buf.at[slot], wq_buf.at[slot], sem_wq.at[slot]).wait()

    def start_down(j, slot, n=NC):
        for c in down_copies(j, slot, n):
            c.start()

    def forward(k):
        to_par(k).wait_recv()
        fwd(k).start()

    everyone = slice(None)

    def next_q(k):
        start_q(k + SLOTS, k)

    def next_u(k):
        u_copy(k + SLOTS, k).start()

    def wait_rows(k):
        to_sib(k).wait_recv()
        fwd(k).wait_recv()

    @pl.loop(0, 3)
    def _(k):
        to_sib(k).wait_recv()
        wait_q(k, k)
        u_copy(k, k).wait()

        @pl.when(k + 3 < SLOTS)
        def _():
            start_up(k + 3, k + 3)

        q_pass([(k, k)], near)
        u_pass([(k, k)], near)
        forward(k + k // 2)

        @pl.when(k == 1)
        def _():
            fwd(0).wait_recv()
            q_pass([(0, 0)], far)
            u_pass([(0, 0)], far)
            next_q(0)
            next_u(0)
            forward(2)

    fwd(1).wait_recv()
    fwd(2).wait_recv()
    q_pass([(1, 1), (2, 2)], far)
    u_pass([(1, 1), (2, 2)], far)
    next_q(1)
    next_u(1)
    next_q(2)
    next_u(2)
    forward(4)

    @pl.loop(3, SLOTS)
    def _(k):
        wait_rows(k)
        wait_q(k, k)
        u_copy(k, k).wait()
        q_pass([(k, k)], everyone)
        u_pass([(k, k)], everyone)
        next_q(k)

        @pl.when(k == 4)
        def _():
            next_u(3)
            next_u(4)

        forward(2 * k - 1)
        forward(2 * k)

    for k in (5, 6):
        wait_rows(k)
        wait_q(k, k - SLOTS)
        u_copy(k, k - SLOTS).wait()
    q_pass([(5, 0), (6, 1)], everyone)
    u_pass([(5, 0), (6, 1)], far)
    start_down(0, 0)
    start_down(1, 1)
    forward(9)
    for k in (7, 8):
        wait_rows(k)
        wait_q(k, k - SLOTS)
    u_copy(7, 2).wait()
    q_pass([(7, 2), (8, 3)], everyone)
    u_pass([(7, 2)], far)
    start_down(2, 2)
    start_down(3, 3)
    wait_rows(9)
    wait_q(9, 4)
    u_copy(8, 3).wait()
    u_copy(9, 4).wait()
    q_pass([(9, 4)], everyone)

    def attention(qr):
        for h in range(heads):
            o = h * 3 * head_dim
            q = acc_qkv[qr, o:o + head_dim].astype(BF16)
            kk = acc_qkv[:, o + head_dim:o + 2 * head_dim].astype(BF16)
            vv = acc_qkv[:, o + 2 * head_dim:o + 3 * head_dim].astype(BF16)
            s = lax.dot_general(q, kk, (((1,), (1,)), ((), ())), preferred_element_type=F32) * scale
            e = jnp.exp(s - jnp.max(s, axis=-1, keepdims=True))
            l = jnp.sum(e, axis=-1, keepdims=True)
            ov = jnp.dot(e.astype(BF16), vv, preferred_element_type=F32)
            act[qr, h * head_dim:(h + 1) * head_dim] = (ov / l).astype(BF16)


    def product(slot, r, n):
        w = wq_buf[slot, 0:n_out, :, 0:n].reshape(att + ff, n)
        return jnp.dot(act[r], w, preferred_element_type=F32)

    def cross(j, slot, n=NC):
        p = product(slot, far, n)
        snd_x[j, :, 0:n] = p[0:rows]
        snd_sc[j, :, 0:n] = p[rows:2 * rows]
        rs_cross(j, n).start()

    def own(j, slot, n=NC):
        p = product(slot, near, n)
        mine[j, :, 0:n] = p[0:rows]
        snd_so[j, :, 0:n] = p[rows:2 * rows]
        rs_own(j, n).start()

    def combine(j, n=NC):
        rs_cross(j, n).wait_recv()
        snd_x[j, :, 0:n] = snd_x[j, :, 0:n] + rcv_sc[j, :, 0:n]
        rs_x(j, n).start()

    def wait_down(j, slot, n=NC):
        part = wq_buf.at[slot, pl.ds(0, n_out), :, pl.ds(0, n)]
        pltpu.make_async_copy(part, part, sem_wd.at[slot]).wait()

    u_pass([(8, 3), (9, 4)], far, True)
    attention(far)
    start_down(4, 4)

    wait_down(0, 0)
    cross(0, 0)
    u_pass([(5, 0), (6, 1)], near)
    combine(0)
    wait_down(1, 1)
    cross(1, 1)
    u_pass([(7, 2), (8, 3)], near)
    combine(1)
    wait_down(2, 2)
    cross(2, 2)
    u_pass([(9, 4)], near, True)
    attention(near)
    combine(2)

    def refill_down(j):
        slot = j % SLOTS

        @pl.when(j + SLOTS < last)
        def _():
            start_down(j + SLOTS, slot)

        @pl.when(j + SLOTS == last)
        def _():
            start_down(last, slot, n_last)

    wait_down(3, 3)
    cross(3, 3)
    own(0, 0)
    combine(3)
    refill_down(0)

    @pl.loop(4, last)
    def _(j):
        wait_down(j, j % SLOTS)
        cross(j, j % SLOTS)
        own(j - 3, (j - 3) % SLOTS)
        combine(j)
        refill_down(j - 3)

    wait_down(last, last % SLOTS, n_last)
    cross(last, last % SLOTS, n_last)
    own(last - 3, (last - 3) % SLOTS)
    combine(last, n_last)

    @pl.loop(last - 2, last)
    def _(j):
        own(j, j % SLOTS)

    own(last, last % SLOTS, n_last)

    def all_rows(r):
        return xn.at[:, blk(r), :]

    remote(all_rows(0), all_rows(1), s_sib, r_sib.at[0], sib).wait_send()
    remote(all_rows(0), all_rows(2), s_par, r_par.at[0], par).wait_send()
    remote(all_rows(2), all_rows(3), s_fwd, r_fwd.at[0], sib).wait_send()
    full = pl.ds(0, last)
    own_all = remote(snd_so.at[full], rcv_so.at[full], s_ro.at[0], r_ro.at[0], sib)
    remote(snd_sc.at[full], rcv_sc.at[full], s_rc.at[0], r_rc.at[0], sib).wait_send()
    rs_cross(last, n_last).wait_send()
    own_all.wait_send()
    rs_own(last, n_last).wait_send()
    own_all.wait_recv()
    rs_own(last, n_last).wait_recv()

    for j in range(nj):
        n = n_last if j == last else NC
        cols = slice(j * NC, j * NC + n)
        part = x_ref[:, cols].astype(F32) + (mine[j, :, 0:n] + rcv_so[j, :, 0:n])
        rs_x(j, n).wait_recv()
        y_ref[:, cols] = (part + rcv_x[j, :, 0:n]).astype(BF16)

    remote(snd_x.at[full], rcv_x.at[full], s_rx.at[0], r_rx.at[0], par).wait_send()
    rs_x(last, n_last).wait_send()


def solution(mesh):
    def local_block(x_loc, ln_gamma, w_qkv, w_out, w_up, w_down):
        rows, dim = x_loc.shape
        heads, hd3 = w_qkv.shape[1:]
        hd = hd3 // 3
        att = heads * hd
        ff = w_up.shape[1]
        seq = 4 * rows
        nk, nj = dim // KC, pl.cdiv(dim, NC)
        vm = pl.BlockSpec(memory_space=pltpu.VMEM)
        hbm = pl.BlockSpec(memory_space=pl.ANY)
        dma = pltpu.SemaphoreType.DMA
        return pl.pallas_call(
            kernel,
            out_shape=pltpu.VMEM((rows, dim), BF16),
            in_specs=[hbm, hbm, hbm, hbm, hbm, hbm],
            out_specs=vm,
            scratch_shapes=[
                pltpu.VMEM((rows, dim), BF16),
                pltpu.VMEM((1, dim), F32),
                pltpu.VMEM((2, rows, 1), F32),
                pltpu.VMEM((nk, seq, KC), BF16),
                pltpu.VMEM((seq, heads * hd3), F32),
                pltpu.VMEM((seq, ff), F32),
                pltpu.VMEM((SLOTS, heads * KC // hd, hd, hd3), BF16),
                pltpu.VMEM((SLOTS, KC, ff), BF16),
                pltpu.VMEM((seq, att + ff), BF16),
                pltpu.VMEM((nj, rows, NC), F32),
                pltpu.VMEM((nj, rows, NC), F32),
                pltpu.VMEM((nj, rows, NC), F32),
                pltpu.VMEM((nj, rows, NC), F32),
                pltpu.VMEM((nj, rows, NC), F32),
                pltpu.VMEM((nj, rows, NC), F32),
                pltpu.VMEM((nj, rows, NC), F32),
                dma, dma, dma((SLOTS,)), dma((SLOTS,)), dma((SLOTS,)),
                dma, dma((nk,)), dma, dma((nk,)), dma, dma((nk,)),
                dma((2,)), dma((nj,)), dma((2,)), dma((2,)), dma((2,)), dma((nj,)),
            ],
            compiler_params=pltpu.CompilerParams(
                collective_id=0, has_side_effects=True, vmem_limit_bytes=66_000_000),
            cost_estimate=pl.CostEstimate(flops=32 * 10**9, bytes_accessed=125 * 10**6, transcendentals=10**6),
            name="block",
        )(x_loc, ln_gamma.reshape(1, dim), jnp.transpose(w_qkv, (1, 0, 2)).reshape(heads, dim // hd, hd, hd3), w_up,
          w_out, w_down.reshape(ff // hd, hd, dim))

    row_spec = P(("data", "tp"), None)
    return jax.shard_map(
        local_block, mesh=mesh,
        in_specs=(row_spec, P(None), P(None, "tp", None), P("tp", None, None), P(None, "tp"), P("tp", None)),
        out_specs=row_spec, check_vma=False)
```

```python
import jax
import jax.numpy as jnp
from jax import lax
from jax.experimental import pallas as pl
from jax.experimental.pallas import tpu as pltpu
from jax.sharding import PartitionSpec as P

LN_EPS = 1e-6
MESH = pl.DeviceIdType.MESH
F32 = jnp.float32
BF16 = jnp.bfloat16

KC = 512
NC = 384
SLOTS = 5


def kernel(x_hbm, g_hbm, wqkv_ref, wup_ref, wout_ref, wdown_ref, y_ref,
           x_ref, g_ref, stat, xn, acc_qkv, acc_up, wq_buf, wu_buf, act,
           snd_sc, rcv_sc, snd_so, rcv_so, snd_x, rcv_x, mine,
           sem_in, sem_g, sem_wq, sem_wu, sem_wd,
           s_sib, r_sib, s_par, r_par, s_fwd, r_fwd,
           s_rc, r_rc, s_ro, r_ro, s_rx, r_rx):
    rows, dim = x_ref.shape
    heads, head_dim = wout_ref.shape[:2]
    ff = wup_ref.shape[1]
    att = heads * head_dim
    nk, nj = dim // KC, pl.cdiv(dim, NC)
    last, n_last = nj - 1, dim - (nj - 1) * NC
    ksub, n_out = KC // head_dim, (att + ff) // head_dim
    d = lax.axis_index("data")
    t = lax.axis_index("tp")
    sib = (d, t + 1 - 2 * (t % 2))
    par = (d, (t + 2) % 4)
    scale = head_dim ** -0.5
    near, far = slice(0, 2 * rows), slice(2 * rows, 4 * rows)

    x_in = pltpu.make_async_copy(x_hbm, x_ref, sem_in)
    x_in.start()
    g_in = pltpu.make_async_copy(g_hbm, g_ref, sem_g)
    g_in.start()

    bar = pltpu.get_barrier_semaphore()
    for peer in (sib, par):
        pl.semaphore_signal(bar, inc=1, device_id=peer, device_id_type=MESH)

    def q_copies(k, slot):
        return [pltpu.make_async_copy(
            wqkv_ref.at[h, pl.ds(k * ksub, ksub)], wq_buf.at[slot, pl.ds(h * ksub, ksub)], sem_wq.at[slot])
            for h in range(heads)]

    def u_copy(k, slot):
        return pltpu.make_async_copy(wup_ref.at[pl.ds(k * KC, KC), :], wu_buf.at[slot], sem_wu.at[slot])

    def down_copies(j, slot, n=NC):
        src, dst = pl.ds(j * NC, n), pl.ds(0, n)
        return (
            pltpu.make_async_copy(wout_ref.at[:, :, src], wq_buf.at[slot, pl.ds(0, heads), :, dst], sem_wd.at[slot]),
            pltpu.make_async_copy(
                wdown_ref.at[:, :, src], wq_buf.at[slot, pl.ds(heads, n_out - heads), :, dst], sem_wd.at[slot]),
        )

    def remote(src, dst, ssem, rsem, peer):
        return pltpu.make_async_remote_copy(
            src_ref=src, dst_ref=dst, send_sem=ssem, recv_sem=rsem,
            device_id=peer, device_id_type=MESH)

    def blk(r):
        return pl.ds(r * rows, rows)

    def to_sib(k):
        return remote(xn.at[k, blk(0), :], xn.at[k, blk(1), :], s_sib, r_sib.at[k - (k - 3) * ((k + 7) // 10)], sib)

    def to_par(k):
        return remote(xn.at[k, blk(0), :], xn.at[k, blk(2), :], s_par, r_par.at[k], par)

    def fwd(k):
        return remote(xn.at[k, blk(2), :], xn.at[k, blk(3), :], s_fwd, r_fwd.at[k], sib)

    def rs_cross(j, n=NC):
        c = pl.ds(0, n)
        return remote(snd_sc.at[j, :, c], rcv_sc.at[j, :, c], s_rc.at[j // last], r_rc.at[j], sib)

    def rs_own(j, n=NC):
        c = pl.ds(0, n)
        return remote(snd_so.at[j, :, c], rcv_so.at[j, :, c], s_ro.at[j // last], r_ro.at[j // last], sib)

    def rs_x(j, n=NC):
        c = pl.ds(0, n)
        return remote(snd_x.at[j, :, c], rcv_x.at[j, :, c], s_rx.at[j // last], r_rx.at[j // 10 * (j - 9)], par)

    def start_up(k, slot):
        for c in q_copies(k, slot) + [u_copy(k, slot)]:
            c.start()

    start_up(0, 0)

    x_in.wait()
    for i in range(rows // 16):
        r = slice(i * 16, (i + 1) * 16)
        v = x_ref[r, :].astype(F32)
        mean = jnp.mean(v, axis=-1, keepdims=True)
        cen = v - mean
        var = jnp.mean(cen * cen, axis=-1, keepdims=True)
        stat[0, r, :] = mean
        stat[1, r, :] = lax.rsqrt(var + LN_EPS)

    start_up(1, 1)

    def normalize(k):
        c = slice(k * KC, (k + 1) * KC)
        cen = x_ref[:, c].astype(F32) - stat[0]
        xn[k, 0:rows, :] = (cen * stat[1] * g_ref[:, c]).astype(BF16)

    def send(k):
        to_par(k).start()
        to_sib(k).start()

    g_in.wait()
    normalize(0)
    pl.semaphore_wait(bar, 2)
    for k in range(1, nk):
        normalize(k)
        send(k - 1)
    acc_qkv[near] = jnp.zeros_like(acc_qkv[near])
    send(nk - 1)
    acc_qkv[far] = jnp.zeros_like(acc_qkv[far])
    acc_up[...] = jnp.zeros_like(acc_up)

    pair = 2 * 3 * head_dim

    def ksum(terms):
        return sum(jnp.dot(x, w, preferred_element_type=F32) for x, w in terms)

    def q_pass(ks, r):
        for h in range(0, heads, 2):
            sl = slice(h // 2 * pair, (h // 2 + 1) * pair)
            acc_qkv[r, sl] += ksum(
                (xn[k, r, :], jnp.concatenate(
                    [wq_buf[slot, i * ksub:(i + 1) * ksub].reshape(KC, 3 * head_dim) for i in (h, h + 1)], axis=1))
                for k, slot in ks)

    def u_pass(ks, r, final=False):
        for n in range(0, ff, pair):
            end = min(n + pair, ff)
            total = acc_up[r, n:end] + ksum((xn[k, r, :], wu_buf[slot, :, n:end]) for k, slot in ks)
            if final:
                act[r, att + n:att + end] = jax.nn.gelu(total, approximate=True).astype(BF16)
            else:
                acc_up[r, n:end] = total

    def start_q(k, slot):
        for c in q_copies(k, slot):
            c.start()

    def wait_q(k, slot):
        pltpu.make_async_copy(wq_buf.at[slot], wq_buf.at[slot], sem_wq.at[slot]).wait()

    def start_down(j, slot, n=NC):
        for c in down_copies(j, slot, n):
            c.start()

    def forward(k):
        to_par(k).wait_recv()
        fwd(k).start()

    everyone = slice(None)

    def next_q(k):
        start_q(k + SLOTS, k)

    def next_u(k):
        u_copy(k + SLOTS, k).start()

    late = pl.ds(3, nk - 3)
    late_sib = remote(xn.at[late, blk(0), :], xn.at[late, blk(1), :], s_sib, r_sib.at[3], sib)

    def wait_rows(k):
        fwd(k).wait_recv()

    @pl.loop(0, 3)
    def _(k):
        to_sib(k).wait_recv()
        wait_q(k, k)
        u_copy(k, k).wait()

        start_up(k + 2, k + 2)
        q_pass([(k, k)], near)
        u_pass([(k, k)], near)
        forward(k + k // 2)

        @pl.when(k == 1)
        def _():
            fwd(0).wait_recv()
            q_pass([(0, 0)], far)
            u_pass([(0, 0)], far)
            next_q(0)
            next_u(0)
            forward(2)

    fwd(1).wait_recv()
    fwd(2).wait_recv()
    q_pass([(1, 1), (2, 2)], far)
    u_pass([(1, 1), (2, 2)], far)
    next_q(1)
    next_u(1)
    forward(4)
    late_sib.wait_recv()

    @pl.loop(3, SLOTS)
    def _(k):
        wait_rows(k)
        wait_q(k, k)
        u_copy(k, k).wait()
        q_pass([(k, k)], everyone)
        u_pass([(k, k)], everyone)

        @pl.when(k == 3)
        def _():
            next_q(2)
            next_u(2)

        next_q(k)

        @pl.when(k == 4)
        def _():
            next_u(3)
            next_u(4)

        forward(2 * k - 1)
        forward(2 * k)

    for k in (5, 6):
        wait_rows(k)
        wait_q(k, k - SLOTS)
        u_copy(k, k - SLOTS).wait()
    q_pass([(5, 0), (6, 1)], everyone)
    u_pass([(5, 0), (6, 1)], far)
    start_down(0, 0)
    start_down(1, 1)
    forward(9)
    for k in (7, 8):
        wait_rows(k)
        wait_q(k, k - SLOTS)
    u_copy(7, 2).wait()
    q_pass([(7, 2), (8, 3)], everyone)
    u_pass([(7, 2)], far)
    start_down(2, 2)
    start_down(3, 3)
    wait_rows(9)
    wait_q(9, 4)
    u_copy(8, 3).wait()
    u_copy(9, 4).wait()
    q_pass([(9, 4)], everyone)

    def attention(qr):
        for h in range(heads):
            o = h * 3 * head_dim
            q = acc_qkv[qr, o:o + head_dim].astype(BF16)
            kk = acc_qkv[:, o + head_dim:o + 2 * head_dim].astype(BF16)
            vv = acc_qkv[:, o + 2 * head_dim:o + 3 * head_dim].astype(BF16)
            s = lax.dot_general(q, kk, (((1,), (1,)), ((), ())), preferred_element_type=F32) * scale
            e = jnp.exp(s - jnp.max(s, axis=-1, keepdims=True))
            l = jnp.sum(e, axis=-1, keepdims=True)
            ov = jnp.dot(e.astype(BF16), vv, preferred_element_type=F32)
            act[qr, h * head_dim:(h + 1) * head_dim] = (ov / l).astype(BF16)


    def product(slot, r, n):
        w = wq_buf[slot, 0:n_out, :, 0:n].reshape(att + ff, n)
        return jnp.dot(act[r], w, preferred_element_type=F32)

    def cross(j, slot, n=NC):
        p = product(slot, far, n)
        snd_x[j, :, 0:n] = p[0:rows]
        snd_sc[j, :, 0:n] = p[rows:2 * rows]
        rs_cross(j, n).start()

    def own(j, slot, n=NC):
        p = product(slot, near, n)
        mine[j, :, 0:n] = p[0:rows]
        snd_so[j, :, 0:n] = p[rows:2 * rows]
        rs_own(j, n).start()

    def combine(j, n=NC):
        rs_cross(j, n).wait_recv()
        snd_x[j, :, 0:n] = snd_x[j, :, 0:n] + rcv_sc[j, :, 0:n]
        rs_x(j, n).start()

    def wait_down(j, slot, n=NC):
        part = wq_buf.at[slot, pl.ds(0, n_out), :, pl.ds(0, n)]
        pltpu.make_async_copy(part, part, sem_wd.at[slot]).wait()

    u_pass([(8, 3), (9, 4)], far, True)
    attention(far)
    start_down(4, 4)

    wait_down(0, 0)
    cross(0, 0)
    u_pass([(5, 0), (6, 1)], near)
    combine(0)
    wait_down(1, 1)
    cross(1, 1)
    u_pass([(7, 2), (8, 3)], near)
    combine(1)
    wait_down(2, 2)
    cross(2, 2)
    u_pass([(9, 4)], near, True)
    attention(near)
    combine(2)

    def refill_down(j):
        slot = j % SLOTS

        @pl.when(j + SLOTS < last)
        def _():
            start_down(j + SLOTS, slot)

        @pl.when(j + SLOTS == last)
        def _():
            start_down(last, slot, n_last)

    wait_down(3, 3)
    cross(3, 3)
    own(0, 0)
    combine(3)
    refill_down(0)

    @pl.loop(4, last)
    def _(j):
        wait_down(j, j % SLOTS)
        cross(j, j % SLOTS)
        own(j - 3, (j - 3) % SLOTS)
        combine(j)
        refill_down(j - 3)

    wait_down(last, last % SLOTS, n_last)
    cross(last, last % SLOTS, n_last)
    own(last - 3, (last - 3) % SLOTS)
    combine(last, n_last)

    @pl.loop(last - 2, last)
    def _(j):
        own(j, j % SLOTS)

    own(last, last % SLOTS, n_last)

    def all_rows(r):
        return xn.at[:, blk(r), :]

    remote(all_rows(0), all_rows(1), s_sib, r_sib.at[0], sib).wait_send()
    remote(all_rows(0), all_rows(2), s_par, r_par.at[0], par).wait_send()
    remote(all_rows(2), all_rows(3), s_fwd, r_fwd.at[0], sib).wait_send()
    full = pl.ds(0, last)
    own_all = remote(snd_so.at[full], rcv_so.at[full], s_ro.at[0], r_ro.at[0], sib)
    remote(snd_sc.at[full], rcv_sc.at[full], s_rc.at[0], r_rc.at[0], sib).wait_send()
    rs_cross(last, n_last).wait_send()
    own_all.wait_send()
    rs_own(last, n_last).wait_send()
    own_all.wait_recv()
    rs_own(last, n_last).wait_recv()

    ten = pl.ds(0, 10)
    remote(snd_x.at[ten], rcv_x.at[ten], s_rx.at[0], r_rx.at[0], par).wait_recv()
    for j in range(nj):
        n = n_last if j == last else NC
        cols = slice(j * NC, j * NC + n)
        part = x_ref[:, cols].astype(F32) + (mine[j, :, 0:n] + rcv_so[j, :, 0:n])
        if j >= 10:
            rs_x(j, n).wait_recv()
        y_ref[:, cols] = (part + rcv_x[j, :, 0:n]).astype(BF16)

    remote(snd_x.at[full], rcv_x.at[full], s_rx.at[0], r_rx.at[0], par).wait_send()
    rs_x(last, n_last).wait_send()


def solution(mesh):
    def local_block(x_loc, ln_gamma, w_qkv, w_out, w_up, w_down):
        rows, dim = x_loc.shape
        heads, hd3 = w_qkv.shape[1:]
        hd = hd3 // 3
        att = heads * hd
        ff = w_up.shape[1]
        seq = 4 * rows
        nk, nj = dim // KC, pl.cdiv(dim, NC)
        vm = pl.BlockSpec(memory_space=pltpu.VMEM)
        hbm = pl.BlockSpec(memory_space=pl.ANY)
        dma = pltpu.SemaphoreType.DMA
        return pl.pallas_call(
            kernel,
            out_shape=pltpu.VMEM((rows, dim), BF16),
            in_specs=[hbm, hbm, hbm, hbm, hbm, hbm],
            out_specs=vm,
            scratch_shapes=[
                pltpu.VMEM((rows, dim), BF16),
                pltpu.VMEM((1, dim), F32),
                pltpu.VMEM((2, rows, 1), F32),
                pltpu.VMEM((nk, seq, KC), BF16),
                pltpu.VMEM((seq, heads * hd3), F32),
                pltpu.VMEM((seq, ff), F32),
                pltpu.VMEM((SLOTS, heads * KC // hd, hd, hd3), BF16),
                pltpu.VMEM((SLOTS, KC, ff), BF16),
                pltpu.VMEM((seq, att + ff), BF16),
                pltpu.VMEM((nj, rows, NC), F32),
                pltpu.VMEM((nj, rows, NC), F32),
                pltpu.VMEM((nj, rows, NC), F32),
                pltpu.VMEM((nj, rows, NC), F32),
                pltpu.VMEM((nj, rows, NC), F32),
                pltpu.VMEM((nj, rows, NC), F32),
                pltpu.VMEM((nj, rows, NC), F32),
                dma, dma, dma((SLOTS,)), dma((SLOTS,)), dma((SLOTS,)),
                dma, dma((4,)), dma, dma((nk,)), dma, dma((nk,)),
                dma((2,)), dma((nj,)), dma((2,)), dma((2,)), dma((2,)), dma((nj - 9,)),
            ],
            compiler_params=pltpu.CompilerParams(
                collective_id=0, has_side_effects=True, vmem_limit_bytes=66_000_000),
            cost_estimate=pl.CostEstimate(flops=32 * 10**9, bytes_accessed=125 * 10**6, transcendentals=10**6),
            name="block",
        )(x_loc, ln_gamma.reshape(1, dim), jnp.transpose(w_qkv, (1, 0, 2)).reshape(heads, dim // hd, hd, hd3), w_up,
          w_out, w_down.reshape(ff // hd, hd, dim))

    row_spec = P(("data", "tp"), None)
    return jax.shard_map(
        local_block, mesh=mesh,
        in_specs=(row_spec, P(None), P(None, "tp", None), P("tp", None, None), P(None, "tp"), P("tp", None)),
        out_specs=row_spec, check_vma=False)
```

```python
import jax
import jax.numpy as jnp
from jax import lax
from jax.experimental import pallas as pl
from jax.experimental.pallas import tpu as pltpu
from jax.sharding import PartitionSpec as P

LN_EPS = 1e-6
MESH = pl.DeviceIdType.MESH
F32 = jnp.float32
BF16 = jnp.bfloat16

KC = 512
NC = 384
SLOTS = 5


def kernel(x_hbm, g_hbm, wqkv_ref, wup_ref, wout_ref, wdown_ref, y_ref,
           x_ref, g_ref, stat, xn, acc_qkv, acc_up, wq_buf, wu_buf, act,
           snd_sc, rcv_sc, snd_so, rcv_so, snd_x, rcv_x, mine,
           sem_in, sem_g, sem_wq, sem_wu,
           s_sib, r_sib, s_par, r_par, s_fwd, r_fwd,
           s_rc, r_rc, s_ro, r_ro, s_rx, r_rx):
    rows, dim = x_ref.shape
    heads, head_dim = wout_ref.shape[:2]
    ff = wup_ref.shape[1]
    att = heads * head_dim
    nk, nj = dim // KC, pl.cdiv(dim, NC)
    last, n_last = nj - 1, dim - (nj - 1) * NC
    ksub, n_out = KC // head_dim, (att + ff) // head_dim
    d = lax.axis_index("data")
    t = lax.axis_index("tp")
    sib = (d, t + 1 - 2 * (t % 2))
    par = (d, (t + 2) % 4)
    scale = head_dim ** -0.5
    near, far = slice(0, 2 * rows), slice(2 * rows, 4 * rows)

    x_in = pltpu.make_async_copy(x_hbm, x_ref, sem_in)
    x_in.start()
    g_in = pltpu.make_async_copy(g_hbm, g_ref, sem_g)
    g_in.start()

    bar = pltpu.get_barrier_semaphore()
    for peer in (sib, par):
        pl.semaphore_signal(bar, inc=1, device_id=peer, device_id_type=MESH)

    def q_copies(k, slot):
        return [pltpu.make_async_copy(
            wqkv_ref.at[h, pl.ds(k * ksub, ksub)], wq_buf.at[slot, pl.ds(h * ksub, ksub)], sem_wq.at[slot])
            for h in range(heads)]

    def u_copy(k, slot):
        return pltpu.make_async_copy(wup_ref.at[pl.ds(k * KC, KC), :], wu_buf.at[slot], sem_wu.at[slot])

    def down_copies(j, slot, n=NC):
        src, dst = pl.ds(j * NC, n), pl.ds(0, n)
        return (
            pltpu.make_async_copy(wout_ref.at[:, :, src], wq_buf.at[slot, pl.ds(0, heads), :, dst], sem_wq.at[slot]),
            pltpu.make_async_copy(
                wdown_ref.at[:, :, src], wq_buf.at[slot, pl.ds(heads, n_out - heads), :, dst], sem_wq.at[slot]),
        )

    def remote(src, dst, ssem, rsem, peer):
        return pltpu.make_async_remote_copy(
            src_ref=src, dst_ref=dst, send_sem=ssem, recv_sem=rsem,
            device_id=peer, device_id_type=MESH)

    def blk(r):
        return pl.ds(r * rows, rows)

    def to_sib(k):
        return remote(xn.at[k, blk(0), :], xn.at[k, blk(1), :], s_sib, r_sib.at[k - (k - 3) * ((k + 7) // 10)], sib)

    def to_par(k):
        return remote(xn.at[k, blk(0), :], xn.at[k, blk(2), :], s_par, r_par.at[k], par)

    def fwd(k):
        return remote(xn.at[k, blk(2), :], xn.at[k, blk(3), :], s_fwd, r_fwd.at[k], sib)

    def rs_cross(j, n=NC):
        c = pl.ds(0, n)
        return remote(snd_sc.at[j, :, c], rcv_sc.at[j, :, c], s_rc.at[j // last], r_rc.at[j], sib)

    def rs_own(j, n=NC):
        c = pl.ds(0, n)
        return remote(snd_so.at[j, :, c], rcv_so.at[j, :, c], s_ro.at[j // last], r_ro.at[j // last], sib)

    def rs_x(j, n=NC):
        c = pl.ds(0, n)
        return remote(snd_x.at[j, :, c], rcv_x.at[j, :, c], s_rx.at[j // last], r_rx.at[j // 10 * (j - 9)], par)

    def start_up(k, slot):
        for c in q_copies(k, slot) + [u_copy(k, slot)]:
            c.start()

    start_up(0, 0)

    x_in.wait()
    for i in range(rows // 16):
        r = slice(i * 16, (i + 1) * 16)
        v = x_ref[r, :].astype(F32)
        mean = jnp.mean(v, axis=-1, keepdims=True)
        cen = v - mean
        var = jnp.mean(cen * cen, axis=-1, keepdims=True)
        stat[0, r, :] = mean
        stat[1, r, :] = lax.rsqrt(var + LN_EPS)

    start_up(1, 1)

    def normalize(k):
        c = slice(k * KC, (k + 1) * KC)
        cen = x_ref[:, c].astype(F32) - stat[0]
        xn[k, 0:rows, :] = (cen * stat[1] * g_ref[:, c]).astype(BF16)

    def send(k):
        to_par(k).start()
        to_sib(k).start()

    g_in.wait()
    normalize(0)
    pl.semaphore_wait(bar, 2)
    for k in range(1, nk):
        normalize(k)
        send(k - 1)
    acc_qkv[near] = jnp.zeros_like(acc_qkv[near])
    send(nk - 1)
    acc_qkv[far] = jnp.zeros_like(acc_qkv[far])
    acc_up[...] = jnp.zeros_like(acc_up)

    pair = 2 * 3 * head_dim

    def ksum(terms):
        return sum(jnp.dot(x, w, preferred_element_type=F32) for x, w in terms)

    def q_pass(ks, r):
        for h in range(0, heads, 2):
            sl = slice(h // 2 * pair, (h // 2 + 1) * pair)
            acc_qkv[r, sl] += ksum(
                (xn[k, r, :], jnp.concatenate(
                    [wq_buf[slot, i * ksub:(i + 1) * ksub].reshape(KC, 3 * head_dim) for i in (h, h + 1)], axis=1))
                for k, slot in ks)

    def u_pass(ks, r, final=False):
        for n in range(0, ff, pair):
            end = min(n + pair, ff)
            total = acc_up[r, n:end] + ksum((xn[k, r, :], wu_buf[slot, :, n:end]) for k, slot in ks)
            if final:
                act[r, att + n:att + end] = jax.nn.gelu(total, approximate=True).astype(BF16)
            else:
                acc_up[r, n:end] = total

    def start_q(k, slot):
        for c in q_copies(k, slot):
            c.start()

    def wait_q(k, slot):
        pltpu.make_async_copy(wq_buf.at[slot], wq_buf.at[slot], sem_wq.at[slot]).wait()

    def start_down(j, slot, n=NC):
        for c in down_copies(j, slot, n):
            c.start()

    def forward(k):
        to_par(k).wait_recv()
        fwd(k).start()

    everyone = slice(None)

    def next_q(k):
        start_q(k + SLOTS, k)

    def next_u(k):
        u_copy(k + SLOTS, k).start()

    late = pl.ds(3, nk - 3)
    late_sib = remote(xn.at[late, blk(0), :], xn.at[late, blk(1), :], s_sib, r_sib.at[3], sib)

    def wait_rows(k):
        fwd(k).wait_recv()

    @pl.loop(0, 3)
    def _(k):
        to_sib(k).wait_recv()
        wait_q(k, k)
        u_copy(k, k).wait()

        start_up(k + 2, k + 2)
        q_pass([(k, k)], near)
        u_pass([(k, k)], near)
        forward(k + k // 2)

        @pl.when(k == 1)
        def _():
            fwd(0).wait_recv()
            q_pass([(0, 0)], far)
            u_pass([(0, 0)], far)
            next_q(0)
            next_u(0)
            forward(2)

    fwd(1).wait_recv()
    fwd(2).wait_recv()
    q_pass([(1, 1), (2, 2)], far)
    u_pass([(1, 1), (2, 2)], far)
    next_q(1)
    next_u(1)
    forward(4)
    late_sib.wait_recv()

    @pl.loop(3, SLOTS)
    def _(k):
        wait_rows(k)
        wait_q(k, k)
        u_copy(k, k).wait()
        q_pass([(k, k)], everyone)
        u_pass([(k, k)], everyone)

        @pl.when(k == 3)
        def _():
            next_q(2)
            next_u(2)

        next_q(k)

        @pl.when(k == 4)
        def _():
            next_u(3)
            next_u(4)

        forward(2 * k - 1)
        forward(2 * k)

    for k in (5, 6):
        wait_rows(k)
        wait_q(k, k - SLOTS)
        u_copy(k, k - SLOTS).wait()
    q_pass([(5, 0), (6, 1)], everyone)
    u_pass([(5, 0), (6, 1)], far)
    start_down(0, 0)
    start_down(1, 1)
    forward(9)
    for k in (7, 8):
        wait_rows(k)
        wait_q(k, k - SLOTS)
    u_copy(7, 2).wait()
    q_pass([(7, 2), (8, 3)], everyone)
    u_pass([(7, 2)], far)
    start_down(2, 2)
    start_down(3, 3)
    wait_rows(9)
    wait_q(9, 4)
    u_copy(8, 3).wait()
    u_copy(9, 4).wait()
    q_pass([(9, 4)], everyone)

    def attention(qr):
        for h in range(heads):
            o = h * 3 * head_dim
            q = acc_qkv[qr, o:o + head_dim].astype(BF16)
            kk = acc_qkv[:, o + head_dim:o + 2 * head_dim].astype(BF16)
            vv = acc_qkv[:, o + 2 * head_dim:o + 3 * head_dim].astype(BF16)
            s = lax.dot_general(q, kk, (((1,), (1,)), ((), ())), preferred_element_type=F32) * scale
            e = jnp.exp(s - jnp.max(s, axis=-1, keepdims=True))
            l = jnp.sum(e, axis=-1, keepdims=True)
            ov = jnp.dot(e.astype(BF16), vv, preferred_element_type=F32)
            act[qr, h * head_dim:(h + 1) * head_dim] = (ov / l).astype(BF16)


    def product(slot, r, n):
        w = wq_buf[slot, 0:n_out, :, 0:n].reshape(att + ff, n)
        return jnp.dot(act[r], w, preferred_element_type=F32)

    def cross(j, slot, n=NC):
        p = product(slot, far, n)
        snd_x[j, :, 0:n] = p[0:rows]
        snd_sc[j, :, 0:n] = p[rows:2 * rows]
        rs_cross(j, n).start()

    def own(j, slot, n=NC):
        p = product(slot, near, n)
        mine[j, :, 0:n] = p[0:rows]
        snd_so[j, :, 0:n] = p[rows:2 * rows]
        rs_own(j, n).start()

    def combine(j, n=NC):
        rs_cross(j, n).wait_recv()
        snd_x[j, :, 0:n] = snd_x[j, :, 0:n] + rcv_sc[j, :, 0:n]
        rs_x(j, n).start()

    def wait_down(j, slot, n=NC):
        part = wq_buf.at[slot, pl.ds(0, n_out), :, pl.ds(0, n)]
        pltpu.make_async_copy(part, part, sem_wq.at[slot]).wait()

    u_pass([(8, 3), (9, 4)], far, True)
    attention(far)
    start_down(4, 4)

    wait_down(0, 0)
    cross(0, 0)
    u_pass([(5, 0), (6, 1)], near)
    combine(0)
    wait_down(1, 1)
    cross(1, 1)
    u_pass([(7, 2), (8, 3)], near)
    combine(1)
    wait_down(2, 2)
    cross(2, 2)
    u_pass([(9, 4)], near, True)
    attention(near)
    combine(2)

    def refill_down(j):
        slot = j % SLOTS

        @pl.when(j + SLOTS < last)
        def _():
            start_down(j + SLOTS, slot)

        @pl.when(j + SLOTS == last)
        def _():
            start_down(last, slot, n_last)

    wait_down(3, 3)
    cross(3, 3)
    own(0, 0)
    combine(3)
    refill_down(0)

    @pl.loop(4, last)
    def _(j):
        wait_down(j, j % SLOTS)
        cross(j, j % SLOTS)
        own(j - 3, (j - 3) % SLOTS)
        combine(j)
        refill_down(j - 3)

    wait_down(last, last % SLOTS, n_last)
    cross(last, last % SLOTS, n_last)
    own(last - 3, (last - 3) % SLOTS)
    combine(last, n_last)

    @pl.loop(last - 2, last)
    def _(j):
        own(j, j % SLOTS)

    own(last, last % SLOTS, n_last)

    def all_rows(r):
        return xn.at[:, blk(r), :]

    remote(all_rows(0), all_rows(1), s_sib, r_sib.at[0], sib).wait_send()
    remote(all_rows(0), all_rows(2), s_par, r_par.at[0], par).wait_send()
    remote(all_rows(2), all_rows(3), s_fwd, r_fwd.at[0], sib).wait_send()
    full = pl.ds(0, last)
    own_all = remote(snd_so.at[full], rcv_so.at[full], s_ro.at[0], r_ro.at[0], sib)
    remote(snd_sc.at[full], rcv_sc.at[full], s_rc.at[0], r_rc.at[0], sib).wait_send()
    rs_cross(last, n_last).wait_send()
    own_all.wait_send()
    rs_own(last, n_last).wait_send()
    own_all.wait_recv()
    rs_own(last, n_last).wait_recv()

    ten = pl.ds(0, 10)
    remote(snd_x.at[ten], rcv_x.at[ten], s_rx.at[0], r_rx.at[0], par).wait_recv()
    for j in range(nj):
        n = n_last if j == last else NC
        cols = slice(j * NC, j * NC + n)
        part = x_ref[:, cols].astype(F32) + (mine[j, :, 0:n] + rcv_so[j, :, 0:n])
        if j >= 10:
            rs_x(j, n).wait_recv()
        y_ref[:, cols] = (part + rcv_x[j, :, 0:n]).astype(BF16)

    remote(snd_x.at[full], rcv_x.at[full], s_rx.at[0], r_rx.at[0], par).wait_send()
    rs_x(last, n_last).wait_send()


def solution(mesh):
    def local_block(x_loc, ln_gamma, w_qkv, w_out, w_up, w_down):
        rows, dim = x_loc.shape
        heads, hd3 = w_qkv.shape[1:]
        hd = hd3 // 3
        att = heads * hd
        ff = w_up.shape[1]
        seq = 4 * rows
        nk, nj = dim // KC, pl.cdiv(dim, NC)
        vm = pl.BlockSpec(memory_space=pltpu.VMEM)
        hbm = pl.BlockSpec(memory_space=pl.ANY)
        dma = pltpu.SemaphoreType.DMA
        return pl.pallas_call(
            kernel,
            out_shape=pltpu.VMEM((rows, dim), BF16),
            in_specs=[hbm, hbm, hbm, hbm, hbm, hbm],
            out_specs=vm,
            scratch_shapes=[
                pltpu.VMEM((rows, dim), BF16),
                pltpu.VMEM((1, dim), F32),
                pltpu.VMEM((2, rows, 1), F32),
                pltpu.VMEM((nk, seq, KC), BF16),
                pltpu.VMEM((seq, heads * hd3), F32),
                pltpu.VMEM((seq, ff), F32),
                pltpu.VMEM((SLOTS, heads * KC // hd, hd, hd3), BF16),
                pltpu.VMEM((SLOTS, KC, ff), BF16),
                pltpu.VMEM((seq, att + ff), BF16),
                pltpu.VMEM((nj, rows, NC), F32),
                pltpu.VMEM((nj, rows, NC), F32),
                pltpu.VMEM((nj, rows, NC), F32),
                pltpu.VMEM((nj, rows, NC), F32),
                pltpu.VMEM((nj, rows, NC), F32),
                pltpu.VMEM((nj, rows, NC), F32),
                pltpu.VMEM((nj, rows, NC), F32),
                dma, dma, dma((SLOTS,)), dma((SLOTS,)),
                dma, dma((4,)), dma, dma((nk,)), dma, dma((nk,)),
                dma((2,)), dma((nj,)), dma((2,)), dma((2,)), dma((2,)), dma((nj - 9,)),
            ],
            compiler_params=pltpu.CompilerParams(
                collective_id=0, has_side_effects=True, vmem_limit_bytes=66_000_000),
            cost_estimate=pl.CostEstimate(flops=32 * 10**9, bytes_accessed=125 * 10**6, transcendentals=10**6),
            name="block",
        )(x_loc, ln_gamma.reshape(1, dim), jnp.transpose(w_qkv, (1, 0, 2)).reshape(heads, dim // hd, hd, hd3), w_up,
          w_out, w_down.reshape(ff // hd, hd, dim))

    row_spec = P(("data", "tp"), None)
    return jax.shard_map(
        local_block, mesh=mesh,
        in_specs=(row_spec, P(None), P(None, "tp", None), P("tp", None, None), P(None, "tp"), P("tp", None)),
        out_specs=row_spec, check_vma=False)
```
